32 devices in a mesh: grp: 2 (over y), theta: 8 (over z, x), phi: 2 (over core).
Axes of the slice: x: 2, y: 2, z: 4, core: 2. Of those that a mesh axis runs over, the one named last changes fastest.
Arguments:
- maps: bfloat16 [8, 4096, 4096], P('grp', 'theta', 'phi'), parts along dimension 0, may hold values from -6 to 6
- deltas: bfloat16 [4096, 4, 4096], P('phi', None, 'theta'), may hold values from -1 to 1
- spin_rows: bfloat16 [4096, 2, 4], P('phi'), may hold values from -1 to 1
- ell_index: int32 [4], replicated, may hold values from 1024 to 2047
- owner_map: int32 [4096], replicated, may hold values from 0 to 4095, each once
- prior: float32 [4], replicated, may hold values from 0.3 to 3
Outputs:
- gradient: float32 [8, 2, 4096], P('grp', None, ('theta', 'phi')), parts along dimension 0
The draws below stay inside these ranges and needn't reach their ends.
There are 2 independent parts, one for each index of `grp`. The reference program is written for one: setup_inputs(seed, part) draws one part's arguments, and reference() takes and returns one part's arrays. A program takes and returns all parts, laid end to end along the dimension named above; an argument that names none is the same for every part. Nothing has to cross between parts.
Inputs may be any that keep to these rules, and one draw needn't show every extreme that they name: `ell_index`: every selected degree is at least 1024; tables may repeat a degree. A permutation of the Fourier indices; slot s of deltas and of the output belongs to the frequency owner_map[s].
All inputs are finite; a program needn't handle non-finite values.
Results may differ from the reference program's by a relative error of at most 0.0003.
Values may be sent and summed in bfloat16 or wider, within the bound.
A program may use at most 256 MiB of HBM per device.

```python
import math
import jax
import jax.numpy as jnp
from jax import lax

L = 2048
NL = 4


def touch_ends(result, rng, low, top_value):
    place = [jax.random.randint(jax.random.fold_in(rng, axis), (), 0, length) for axis, length in enumerate(result.shape)]
    longest = result.shape.index(max(result.shape))
    beside = place[:longest] + [(place[longest] + 1) % result.shape[longest]] + place[longest + 1:]
    return result.at[tuple(place)].set(low).at[tuple(beside)].set(top_value)


def shard_levels(rng, dims, shards, low, high):
    factor_of, own = 1.0, jax.random.fold_in(rng, 6)
    for dim, parts in shards:
        steps = jnp.exp(jax.random.uniform(jax.random.fold_in(own, dim), (parts,), jnp.float32, low / len(shards), high / len(shards)))
        factor_of = factor_of * jnp.repeat(steps, dims[dim] // parts).reshape([-1 if axis == dim else 1 for axis in range(len(dims))])
    return factor_of


def bell_draw(rng, dims, width, limit, pieces=(), kind=jnp.bfloat16):
    array = width * jax.random.normal(rng, dims, jnp.float32)
    if pieces:
        array = array * shard_levels(rng, dims, pieces, -0.22, 0.18)
    return jnp.clip(array, -limit, limit).astype(kind)


def setup_inputs(seed: int = 0, part: int = 0) -> dict:
    streams_of = jax.random.split(jax.random.key(seed), 7)
    part_keys = jax.random.split(jax.random.fold_in(streams_of[6], part), 7)
    maps = bell_draw(part_keys[0], (4, 2 * L, 2 * L), 1.0, 6.0, ((1, 8), (2, 2)))
    deltas = jnp.clip(jax.random.uniform(streams_of[1], (2 * L, NL, 2 * L), jnp.float32, -1.0, 1.0) * shard_levels(streams_of[1], (2 * L, NL, 2 * L), ((0, 2), (2, 8)), -0.4, 0.0), -1.0, 1.0).astype(jnp.bfloat16)
    spin_rows = jnp.clip(jax.random.uniform(streams_of[2], (2 * L, 2, NL), jnp.float32, -1.0, 1.0) * shard_levels(streams_of[2], (2 * L, 2, NL), ((0, 2),), -0.4, 0.0), -1.0, 1.0).astype(jnp.bfloat16)
    ell_index = touch_ends(jax.random.randint(streams_of[3], (NL,), L // 2, L), jax.random.fold_in(streams_of[3], 1), L // 2, L - 1).astype(jnp.int32)
    owner_map = jax.random.permutation(streams_of[4], 2 * L).astype(jnp.int32)
    prior = jnp.clip(jnp.exp(jax.random.uniform(streams_of[5], (NL,), jnp.float32, math.log(0.3), math.log(3.0))), 0.3, 3.0)
    return dict(maps=maps, deltas=deltas, spin_rows=spin_rows, ell_index=ell_index, owner_map=owner_map, prior=prior)


def signed_freq(length):
    positions = jnp.arange(length, dtype=jnp.int32)
    return jnp.where(positions < length // 2, positions, positions - length)

def reference(maps, deltas, spin_rows, ell_index, owner_map, prior):
    length = 2 * L
    values = maps.astype(jnp.float32)
    prod_real = values[1] * values[2]
    prod_imag = values[1] * values[3]
    scalar_spec = jnp.fft.fft2(values[0]) / length
    spin_spec = jnp.fft.fft2(lax.complex(prod_real, prod_imag)) / length
    planes = [jnp.real(scalar_spec)[:, owner_map].astype(jnp.float32), jnp.imag(scalar_spec)[:, owner_map].astype(jnp.float32), jnp.real(spin_spec)[:, owner_map].astype(jnp.float32), jnp.imag(spin_spec)[:, owner_map].astype(jnp.float32)]
    freq = signed_freq(length)
    slot_freq = freq[owner_map]
    turns = jnp.mod(-slot_freq, 4)
    phase_real = jnp.where(turns == 0, 1.0, jnp.where(turns == 2, -1.0, 0.0)).astype(jnp.float32)
    phase_imag = jnp.where(turns == 1, 1.0, jnp.where(turns == 3, -1.0, 0.0)).astype(jnp.float32)
    outputs = []
    for degree in range(NL):
        ell = ell_index[degree]
        ell_float = ell.astype(jnp.float32)
        keep_rows = (jnp.abs(freq) <= ell).astype(jnp.float32)
        keep_slots = (jnp.abs(slot_freq) <= ell).astype(jnp.float32)
        table = deltas[:, degree, :].astype(jnp.float32)
        weight = 2.0 * math.pi / length * jnp.sqrt((2.0 * ell_float + 1.0) / (4.0 * math.pi))
        sums = []
        for plane_pos in range(4):
            spin = plane_pos // 2
            row_weights = spin_rows[:, spin, degree].astype(jnp.float32) * keep_rows
            total = jnp.einsum('k,ks->s', row_weights, table * planes[plane_pos], precision=lax.Precision.HIGHEST)
            sums.append(total * weight * keep_slots)
        coupling = prior[degree] * jnp.sqrt(ell_float * (ell_float + 1.0)) / L
        inner_real = -sums[3] - coupling * sums[0]
        inner_imag = sums[2] - coupling * sums[1]
        out_real = phase_real * inner_real - phase_imag * inner_imag
        out_imag = phase_real * inner_imag + phase_imag * inner_real
        outputs.append(jnp.stack([out_real, out_imag]))
    return jnp.stack(outputs)
```

```python
import functools
import math

import jax
import jax.numpy as jnp
import numpy as np
from jax import lax
from jax.experimental import pallas as pl
from jax.experimental.pallas import tpu as pltpu
from jax.sharding import PartitionSpec as P


def exact_einsum(form, table, operand):
    return jnp.einsum(form, table, operand, precision=lax.Precision.HIGHEST)


def angle_tables(row_count, start, count, modulus):
    freq_rows = jnp.arange(row_count, dtype=jnp.int32)
    sample_cols = start + jnp.arange(count, dtype=jnp.int32)
    angles = (
        2.0
        * math.pi
        / modulus
        * jnp.mod(freq_rows[:, None] * sample_cols[None, :], modulus).astype(jnp.float32)
    )
    return (jnp.cos(angles), jnp.sin(angles))


def row_transform(real_part, imag_part, outer_len, inner_len):
    row_count = real_part.shape[0]
    length = outer_len * inner_len
    cos_a, sin_a = angle_tables(outer_len, 0, outer_len, outer_len)
    real_blocks = real_part.reshape(row_count, outer_len, inner_len)
    section_real = exact_einsum("ka,rab->rkb", cos_a, real_blocks)
    section_imag = -exact_einsum("ka,rab->rkb", sin_a, real_blocks)
    if imag_part is not None:
        imag_blocks = imag_part.reshape(row_count, outer_len, inner_len)
        section_real = section_real + exact_einsum("ka,rab->rkb", sin_a, imag_blocks)
        section_imag = section_imag + exact_einsum("ka,rab->rkb", cos_a, imag_blocks)
    cos_t, sin_t = angle_tables(outer_len, 0, inner_len, length)
    turned_real = section_real * cos_t + section_imag * sin_t
    turned_imag = section_imag * cos_t - section_real * sin_t
    cos_b, sin_b = angle_tables(inner_len, 0, inner_len, inner_len)
    out_real = exact_einsum("qb,rkb->rqk", cos_b, turned_real) + exact_einsum(
        "qb,rkb->rqk", sin_b, turned_imag
    )
    out_imag = exact_einsum("qb,rkb->rqk", cos_b, turned_imag) - exact_einsum(
        "qb,rkb->rqk", sin_b, turned_real
    )
    return (out_real.reshape(row_count, length), out_imag.reshape(row_count, length))


def column_transform(real_part, imag_part, outer_len, inner_len, start):
    fields = real_part.shape[0]
    count = real_part.shape[2]
    slots = real_part.shape[3]
    length = outer_len * inner_len
    cos_a, sin_a = angle_tables(outer_len, 0, outer_len, outer_len)
    section_real = exact_einsum("ka,fabm->fkbm", cos_a, real_part) + exact_einsum(
        "ka,fabm->fkbm", sin_a, imag_part
    )
    section_imag = exact_einsum("ka,fabm->fkbm", cos_a, imag_part) - exact_einsum(
        "ka,fabm->fkbm", sin_a, real_part
    )
    cos_t, sin_t = angle_tables(outer_len, start, count, length)
    cos_t = cos_t[:, :, None]
    sin_t = sin_t[:, :, None]
    turned_real = section_real * cos_t + section_imag * sin_t
    turned_imag = section_imag * cos_t - section_real * sin_t
    cos_b, sin_b = angle_tables(inner_len, start, count, inner_len)
    out_real = exact_einsum("qb,fkbm->fqkm", cos_b, turned_real) + exact_einsum(
        "qb,fkbm->fqkm", sin_b, turned_imag
    )
    out_imag = exact_einsum("qb,fkbm->fqkm", cos_b, turned_imag) - exact_einsum(
        "qb,fkbm->fqkm", sin_b, turned_real
    )
    return (out_real.reshape(fields, length, slots), out_imag.reshape(fields, length, slots))


def accumulate(spectrum_block, table_block, spin_block, length, ell_index):
    count = table_block.shape[0]
    positions = jnp.arange(count, dtype=jnp.int32)
    freq = jnp.where(positions < length // 2, positions, positions - length)
    terms = []
    for degree in range(table_block.shape[1]):
        keep_rows = (jnp.abs(freq) <= ell_index[degree]).astype(jnp.float32)
        row_weights = spin_block[:, :, degree].astype(jnp.float32).T * keep_rows[None, :]
        table = table_block[:, degree, :].astype(jnp.float32)
        terms.append(
            jnp.einsum(
                "fk,ks,xfks->fxs",
                row_weights,
                table,
                spectrum_block,
                precision=lax.Precision.HIGHEST,
            )
        )
    return jnp.stack(terms)


def on_device_general(maps, deltas, spin_rows, ell_index, owner_map, prior):
    theta_count = lax.axis_size("theta")
    phi_count = lax.axis_size("phi")
    length = maps.shape[2] * phi_count
    values = maps.astype(jnp.float32)
    planes = jnp.stack([values[0], values[1] * values[2], values[1] * values[3]])
    row_planes = lax.all_to_all(planes, "phi", split_axis=1, concat_axis=2, tiled=True)
    inner_len = length // theta_count
    spectra = [
        row_transform(row_planes[0], None, theta_count, inner_len),
        row_transform(row_planes[1], row_planes[2], theta_count, inner_len),
    ]
    stacked = jnp.stack(
        [
            jnp.stack([spectrum[0] for spectrum in spectra]),
            jnp.stack([spectrum[1] for spectrum in spectra]),
        ]
    )
    permuted = jnp.take(stacked, owner_map, axis=3)
    columns = lax.all_to_all(permuted, "theta", split_axis=3, concat_axis=2, tiled=True)
    fields = columns.shape[1]
    slots = columns.shape[3]
    sub_rows = columns.shape[2] // theta_count
    blocks = columns.reshape(2, fields, theta_count, sub_rows, slots)
    row_start = lax.axis_index("phi") * sub_rows
    spec_real, spec_imag = column_transform(blocks[0], blocks[1], theta_count, inner_len, row_start)
    combined = jnp.stack([spec_real, spec_imag])
    totals = accumulate(
        combined,
        lax.all_gather(deltas, "phi", axis=0, tiled=True),
        lax.all_gather(spin_rows, "phi", axis=0, tiled=True),
        length,
        ell_index,
    )
    shares = lax.psum_scatter(totals, "phi", scatter_dimension=3, tiled=True)
    share_count = shares.shape[3]
    slot_start = lax.axis_index("theta") * slots + lax.axis_index("phi") * share_count
    share_ids = lax.dynamic_slice_in_dim(owner_map, slot_start, share_count)
    slot_freq = jnp.where(share_ids < length // 2, share_ids, share_ids - length)
    ell_float = ell_index.astype(jnp.float32)
    weight = 2.0 * math.pi / length * jnp.sqrt((2.0 * ell_float + 1.0) / (4.0 * math.pi)) / length
    keep_slots = (jnp.abs(slot_freq)[None, :] <= ell_index[:, None]).astype(jnp.float32) * weight[
        :, None
    ]
    scalar_real = shares[:, 0, 0] * keep_slots
    scalar_imag = shares[:, 0, 1] * keep_slots
    spin_real = shares[:, 1, 0] * keep_slots
    spin_imag = shares[:, 1, 1] * keep_slots
    coupling = (prior * jnp.sqrt(ell_float * (ell_float + 1.0)) / (length // 2))[:, None]
    inner_real = -spin_imag - coupling * scalar_real
    inner_imag = spin_real - coupling * scalar_imag
    turns = jnp.mod(-slot_freq, 4)
    phase_real = jnp.where(turns == 0, 1.0, jnp.where(turns == 2, -1.0, 0.0)).astype(jnp.float32)[
        None, :
    ]
    phase_imag = jnp.where(turns == 1, 1.0, jnp.where(turns == 3, -1.0, 0.0)).astype(jnp.float32)[
        None, :
    ]
    out_real = phase_real * inner_real - phase_imag * inner_imag
    out_imag = phase_real * inner_imag + phase_imag * inner_real
    return jnp.stack([out_real, out_imag], axis=1)


ROW_OUTER = 8
LANES = 128
VMEM_LIMIT = 67043328
CODE_TOP = 32767.0
MESH = pl.DeviceIdType.MESH


def cplx_add(x, y):
    return tuple(b if a is None else a if b is None else a + b for a, b in zip(x, y))


def cplx_sub(x, y):
    return tuple(
        (None if b is None else -b) if a is None else a if b is None else a - b
        for a, b in zip(x, y)
    )


def turn(x, step, count):
    real, imag = x
    if step == 0:
        return x
    if 4 * step == count:
        return (imag, None if real is None else -real)
    cos_v = math.cos(2.0 * math.pi * step / count)
    sin_v = math.sin(2.0 * math.pi * step / count)
    if imag is None:
        return (real * cos_v, real * -sin_v)
    if 8 * step == count:
        return ((real + imag) * cos_v, (imag - real) * cos_v)
    if 8 * step == 3 * count:
        return ((imag - real) * sin_v, (real + imag) * -sin_v)
    return (real * cos_v + imag * sin_v, imag * cos_v - real * sin_v)


def butterfly(items):
    count = len(items)
    if count == 1:
        return items
    even, odd = butterfly(items[::2]), butterfly(items[1::2])
    turned = [turn(x, step, count) for step, x in enumerate(odd)]
    return [cplx_add(a, b) for a, b in zip(even, turned)] + [
        cplx_sub(a, b) for a, b in zip(even, turned)
    ]


def split_store(high, low, where, value):
    top = value.astype(jnp.bfloat16)
    high[where] = top
    low[where] = (value - top.astype(jnp.float32)).astype(jnp.bfloat16)


def store_matrix(cos_ref, sin_ref, high, low):
    size = cos_ref.shape[0]
    first, second = slice(0, size), slice(size, 2 * size)
    cos_v, sin_v = cos_ref[...], sin_ref[...]
    split_store(high, low, (first, first), cos_v)
    split_store(high, low, (first, second), sin_v)
    split_store(high, low, (second, first), -sin_v)
    split_store(high, low, (second, second), cos_v)


def dot_nt(left, right):
    return lax.dot_general(
        left, right, (((1,), (1,)), ((), ())), preferred_element_type=jnp.float32
    )


def three_dots(mat_high, mat_low, high, low):
    return dot_nt(mat_high[...], high) + dot_nt(mat_high[...], low) + dot_nt(mat_low[...], high)


def turned(item, cos_v, sin_v):
    real, imag = item
    if imag is None:
        return real * cos_v, real * -sin_v
    return real * cos_v + imag * sin_v, imag * cos_v - real * sin_v


def flip_bits(value, mask, count):
    result, bit = 0, 1
    while bit < count:
        result = result + ((value // bit + mask // bit) % 2) * bit
        bit *= 2
    return result


def pipeline_kernel(
    peers, maps, deltas, spins, places, mirror, order, row_cos, row_sin, row_tc, row_ts,
    col_cos, col_sin, col_tc, col_ts, out_ref, land,
    planes, x_high, x_low, row_mat_high, row_mat_low, col_mat_high, col_mat_low, codes, scales,
    stage, scale_stage, recv, scale_recv, table, raw, spin_land, weights, scale_rows, scale_cols,
    total, plane_send, plane_recv, plane_own, land_send, land_recv, spin_send, spin_recv,
    raw_sem, code_send, code_recv, scale_send, scale_sem, own_sem,
):
    theta, phi = lax.axis_index("theta"), lax.axis_index("phi")
    me = theta * 2 + phi
    other = 1 - phi
    rows = planes.shape[2]
    half = planes.shape[3]
    inner = row_cos.shape[0]
    sub = col_cos.shape[0]
    groups = recv.shape[2]
    degrees = deltas.shape[1]
    slots = groups * LANES
    fold = peers // ROW_OUTER
    parts_per_half = half // inner

    def device(index):
        return {"theta": index // 2, "phi": index % 2}

    barrier = pltpu.get_barrier_semaphore()
    for mask in range(1, peers):
        pl.semaphore_signal(
            barrier, inc=1, device_id=device(flip_bits(me, mask, peers)), device_id_type=MESH
        )
    pl.semaphore_wait(barrier, peers - 1)

    def plane_copy(place):
        return pltpu.make_async_remote_copy(
            src_ref=maps.at[place, pl.ds(pl.multiple_of(other * rows, rows), rows), :],
            dst_ref=planes.at[place, 1],
            send_sem=plane_send.at[place],
            recv_sem=plane_recv.at[place],
            device_id={"phi": other},
            device_id_type=MESH,
        )

    def own_plane(place):
        return pltpu.make_async_copy(
            maps.at[place, pl.ds(pl.multiple_of(phi * rows, rows), rows), :],
            planes.at[place, 0],
            plane_own.at[place],
        )

    for place in range(4):
        plane_copy(place).start()
        own_plane(place).start()
    land_copy = pltpu.make_async_remote_copy(
        src_ref=deltas.at[:, :, pl.ds(pl.multiple_of(other * slots, slots), slots)],
        dst_ref=land,
        send_sem=land_send,
        recv_sem=land_recv,
        device_id={"phi": other},
        device_id_type=MESH,
    )
    land_copy.start()
    spin_copy = pltpu.make_async_remote_copy(
        src_ref=spins,
        dst_ref=spin_land,
        send_sem=spin_send,
        recv_sem=spin_recv,
        device_id={"phi": other},
        device_id_type=MESH,
    )
    spin_copy.start()
    store_matrix(row_cos, row_sin, row_mat_high, row_mat_low)

    sign = (1 - 2 * phi).astype(jnp.float32)

    def row_transform_kernel(places_in, kept):
        for place in places_in:
            own_plane(place).wait()
            plane_copy(place).wait_recv()
        step_rows = 16

        def chunk(step, carry):
            span = pl.ds(pl.multiple_of(step * step_rows, step_rows), step_rows)
            for first in range(0, inner, LANES):

                def part(place, a):
                    start = (a % parts_per_half) * inner + first
                    return planes[
                        place, a // parts_per_half, span, start : start + LANES
                    ].astype(jnp.float32)

                items = []
                for a in range(ROW_OUTER):
                    if len(places_in) == 1:
                        items.append((part(places_in[0], a), None))
                    else:
                        base = part(places_in[0], a)
                        items.append((base * part(places_in[1], a), base * part(places_in[2], a)))
                done = butterfly(items)
                for k in range(kept):
                    cos_k = row_tc[k : k + 1, first : first + LANES]
                    sin_k = row_ts[k : k + 1, first : first + LANES]
                    if k % 2:
                        cos_k, sin_k = cos_k * sign, sin_k * sign
                    real, imag = turned(done[k], cos_k, sin_k)
                    split_store(x_high, x_low, (k, span, slice(first, first + LANES)), real)
                    split_store(
                        x_high, x_low, (k, span, slice(inner + first, inner + first + LANES)), imag
                    )
            return carry

        lax.fori_loop(0, rows // step_rows, chunk, 0)

        def block(k, carry):
            both = three_dots(row_mat_high, row_mat_low, x_high[k], x_low[k])
            real, imag = both[:inner], both[inner:]
            top = jnp.max(jnp.maximum(jnp.abs(real), jnp.abs(imag)), axis=1, keepdims=True)
            top = jnp.maximum(top, 1e-30)
            factor = CODE_TOP / top
            code_real = jnp.round(real * factor).astype(jnp.int32)
            code_imag = jnp.round(imag * factor).astype(jnp.int32)
            span = pl.ds(pl.multiple_of(k * inner, inner), inner)
            codes[span, :] = (code_real << 16) | (code_imag & 0xFFFF)
            scales[span, :] = jnp.broadcast_to(top * (1.0 / CODE_TOP), (inner, LANES))
            return carry

        lax.fori_loop(0, kept, block, 0)

    def code_copy(field, step, source):
        group, n = step // peers, step % peers
        dest = flip_bits(me, peers - 1 - n, peers)
        return pltpu.make_async_remote_copy(
            src_ref=stage.at[field, dest, group],
            dst_ref=recv.at[field, source, group],
            send_sem=code_send.at[field, step],
            recv_sem=code_recv.at[field, source, group],
            device_id=device(dest),
            device_id_type=MESH,
        )

    def scale_copy(field, step, source):
        group, n = step // peers, step % peers
        dest = flip_bits(me, peers - 1 - n, peers)
        return pltpu.make_async_remote_copy(
            src_ref=scale_stage.at[field, dest, group],
            dst_ref=scale_recv.at[field, group, source],
            send_sem=scale_send.at[field, step],
            recv_sem=scale_sem.at[field, source, group],
            device_id=device(dest),
            device_id_type=MESH,
        )

    def own_copy(field, group):
        return pltpu.make_async_copy(
            stage.at[field, me, group], recv.at[field, me, group], own_sem.at[field, group]
        )

    lane = lax.broadcasted_iota(jnp.int32, (1, LANES), 1)
    unroll = 8

    def send_step(field, step):
        @pl.when(step % peers != peers - 1)
        def _():
            code_copy(field, step, me).start()
            scale_copy(field, step, me).start()

        @pl.when(step % peers == peers - 1)
        def _():
            own_copy(field, step // peers).start()

    def gather_and_send(field):
        def step_body(step, carry):
            group, n = step // peers, step % peers
            dest = flip_bits(me, peers - 1 - n, peers)
            first = field * peers * slots + dest * slots + group * LANES

            def rows_body(g, acc):
                base = pl.multiple_of(g * unroll, unroll)
                for u in range(unroll):
                    where = places[first + base + u]
                    stage[field, dest, group, pl.ds(base + u, 1), :] = codes[pl.ds(where, 1), :]
                    acc = jnp.where(lane == base + u, scales[pl.ds(where, 1), :], acc)
                return acc

            acc = lax.fori_loop(0, LANES // unroll, rows_body, jnp.zeros((1, LANES), jnp.float32))
            scale_stage[field, dest, group] = acc

            @pl.when(step > 0)
            def _():
                send_step(field, step - 1)

            return carry

        lax.fori_loop(0, groups * peers, step_body, 0)
        send_step(field, groups * peers - 1)

    row_transform_kernel((0,), ROW_OUTER // 2 + 1)
    gather_and_send(0)
    row_transform_kernel((1, 2, 3), ROW_OUTER)
    gather_and_send(1)

    store_matrix(col_cos, col_sin, col_mat_high, col_mat_low)
    spin_copy.wait_recv()
    eye_row = lax.broadcasted_iota(jnp.int32, (LANES, LANES), 0)
    eye_col = lax.broadcasted_iota(jnp.int32, (LANES, LANES), 1)
    eye = (eye_row == eye_col).astype(jnp.float32).astype(jnp.bfloat16)
    for which, ref in ((phi, spins), (other, spin_land)):
        for first in range(0, half, LANES):
            span = pl.ds(pl.multiple_of(which * half + first, LANES), LANES)
            weights[span, :] = dot_nt(eye, ref[:, first : first + LANES])

    raw_rows = raw.shape[1]
    raw_q = raw_rows // peers
    raw_steps = half // raw_rows

    def raw_copy(ref, lanes, step):
        return pltpu.make_async_copy(
            ref.at[pl.ds(pl.multiple_of(step * raw_rows, raw_rows), raw_rows), :, lanes],
            raw.at[step % 2],
            raw_sem.at[step % 2],
        )

    def reorder(ref, lanes, which):
        raw_copy(ref, lanes, 0).start()

        def body(step, carry):
            @pl.when(step + 1 < raw_steps)
            def _():
                raw_copy(ref, lanes, step + 1).start()

            raw_copy(ref, lanes, step).wait()
            base = pl.multiple_of(which * (sub // 2) + step * raw_q, raw_q)
            for group in range(groups):
                pieces = []
                for top in range(0, raw_rows, raw_rows // 2):
                    source = raw[
                        step % 2, top : top + raw_rows // 2, :, group * LANES : (group + 1) * LANES
                    ].reshape(raw_rows // 2 * degrees, LANES)
                    pieces.append(
                        jnp.dot(order[...], source, preferred_element_type=jnp.float32)
                    )
                small = raw_q // 2
                for k in range(peers):
                    for j in range(degrees):
                        start = (k * degrees + j) * small
                        table[group, k, j, pl.ds(base, raw_q), :] = jnp.concatenate(
                            [piece[start : start + small] for piece in pieces], axis=0
                        ).astype(jnp.bfloat16)
            return carry

        lax.fori_loop(0, raw_steps, body, 0)

    reorder(deltas, pl.ds(pl.multiple_of(phi * slots, slots), slots), phi)
    land_copy.wait_recv()
    reorder(land, pl.ds(0, slots), other)

    scale_rows[...] = jnp.zeros_like(scale_rows)

    def column_block(position, carry):
        field, group = position // groups, position % groups

        def wait_one(n, inner_carry):
            source = flip_bits(me, peers - 1 - n, peers)
            code_copy(field, group * peers + n, source).wait_recv()
            scale_copy(field, group * peers + n, source).wait_recv()
            return inner_carry

        lax.fori_loop(0, peers - 1, wait_one, 0)
        own_copy(field, group).wait()
        scale_recv[field, group, me] = scale_stage[field, me, group]

        for a in range(peers):
            scale_rows[a : a + 1, :] = scale_recv[field, group, a]
        plain = scale_rows[...]
        flips = jnp.where(field == 0, mirror[pl.ds(me * groups + group, 1), :], 1.0)
        scale_cols[0] = plain.T
        scale_cols[1] = (plain * flips).T
        step_rows = 16

        def chunk(step, inner_carry):
            span = pl.ds(pl.multiple_of(step * step_rows, step_rows), step_rows)
            sre, sim = scale_cols[0, span, :], scale_cols[1, span, :]
            for first in range(0, sub, LANES):
                items = []
                for a in range(peers):
                    code = recv[field, a, group, span, first : first + LANES]
                    real = (code >> 16).astype(jnp.float32) * sre[:, a : a + 1]
                    imag = ((code << 16) >> 16).astype(jnp.float32) * sim[:, a : a + 1]
                    items.append((real, imag))
                for k, item in enumerate(butterfly(items)):
                    real, imag = turned(
                        item,
                        col_tc[k : k + 1, first : first + LANES],
                        col_ts[k : k + 1, first : first + LANES],
                    )
                    start = (k % fold) * 2 * sub + first
                    split_store(
                        x_high, x_low, (k // fold, span, slice(start, start + LANES)), real
                    )
                    start = start + sub
                    split_store(
                        x_high, x_low, (k // fold, span, slice(start, start + LANES)), imag
                    )
            return inner_carry

        lax.fori_loop(0, LANES // step_rows, chunk, 0)
        total[...] = jnp.zeros_like(total)

        def block(k2, inner_carry):
            for r in range(fold):
                k = k2 * fold + r
                where = (k2, slice(0, LANES), slice(r * 2 * sub, (r + 1) * 2 * sub))
                both = three_dots(col_mat_high, col_mat_low, x_high[where], x_low[where])
                real, imag = both[:sub], both[sub:]
                eight = weights[pl.ds(k, sub, peers), :]
                four = jnp.where(field == 0, eight[:, :degrees], eight[:, degrees : 2 * degrees])
                for j in range(degrees):
                    weighted = table[group, k, j].astype(jnp.float32) * four[:, j : j + 1]
                    for part, value in enumerate((real, imag)):
                        total[2 * j + part] += jnp.sum(
                            (weighted * value).reshape(sub // 8, 8, LANES), axis=0
                        )
            return inner_carry

        lax.fori_loop(0, ROW_OUTER, block, 0)
        out_ref[field, group] = jnp.sum(total[...], axis=1)
        return carry

    lax.fori_loop(0, 2 * groups, column_block, 0)

    for place in range(4):
        plane_copy(place).wait_send()
    land_copy.wait_send()
    spin_copy.wait_send()

    def finish(n, carry):
        for field in range(2):
            for group in range(groups):
                code_copy(field, group * peers + n, me).wait_send()
                scale_copy(field, group * peers + n, me).wait_send()
        return carry

    lax.fori_loop(0, peers - 1, finish, 0)


def wave_tables(row_ids, col_ids, modulus):
    angles = 2.0 * math.pi / modulus * ((row_ids[:, None] * col_ids[None, :]) % modulus)
    return np.cos(angles).astype(np.float32), np.sin(angles).astype(np.float32)


def signed(ids, length):
    return jnp.where(ids < length // 2, ids, ids - length)


def pipeline_call(peers, maps, deltas, spins, places, mirror):
    fields_in, rows_all, half = maps.shape
    rows = rows_all // 2
    length = 2 * half
    slots = deltas.shape[2] // 2
    degrees = deltas.shape[1]
    groups = slots // LANES
    inner = length // ROW_OUTER
    sub = length // peers
    ids = np.arange(length)
    row_cos, row_sin = wave_tables(ids[:inner], ids[:inner], inner)
    row_tc, row_ts = wave_tables(ids[:ROW_OUTER], ids[:inner], length)
    col_cos, col_sin = wave_tables(ids[:sub], ids[:sub], sub)
    col_tc, col_ts = wave_tables(ids[:peers], ids[:sub], length)
    small = 8
    raw_rows = 2 * small * peers
    target = np.arange(small * peers * degrees)
    k, j, q = target // (degrees * small), target // small % degrees, target % small
    source = (q * peers + k) * degrees + j
    order = jnp.asarray(source[:, None] == target[None, :]).astype(jnp.bfloat16)
    bf, f32 = jnp.bfloat16, jnp.float32
    vmem = pl.BlockSpec(memory_space=pltpu.VMEM)
    anywhere = pl.BlockSpec(memory_space=pl.ANY)
    dma = pltpu.SemaphoreType.DMA
    return pl.pallas_call(
        functools.partial(pipeline_kernel, peers),
        in_specs=[anywhere, anywhere, vmem, pl.BlockSpec(memory_space=pltpu.SMEM)] + [vmem] * 10,
        out_specs=[vmem, anywhere],
        out_shape=[
            jax.ShapeDtypeStruct((2, groups, 2 * degrees, LANES), f32),
            jax.ShapeDtypeStruct((half, degrees, slots), bf),
        ],
        scratch_shapes=[
            pltpu.VMEM((fields_in, 2, rows, half), bf),
            pltpu.VMEM((ROW_OUTER, rows, 2 * inner), bf),
            pltpu.VMEM((ROW_OUTER, rows, 2 * inner), bf),
            pltpu.VMEM((2 * inner, 2 * inner), bf),
            pltpu.VMEM((2 * inner, 2 * inner), bf),
            pltpu.VMEM((2 * sub, 2 * sub), bf),
            pltpu.VMEM((2 * sub, 2 * sub), bf),
            pltpu.VMEM((length, rows), jnp.int32),
            pltpu.VMEM((length, LANES), f32),
            pltpu.VMEM((2, peers, groups, LANES, rows), jnp.int32),
            pltpu.VMEM((2, peers, groups, 1, LANES), f32),
            pltpu.VMEM((2, peers, groups, LANES, rows), jnp.int32),
            pltpu.VMEM((2, groups, peers, 1, LANES), f32),
            pltpu.VMEM((groups, peers, degrees, sub, LANES), bf),
            pltpu.VMEM((2, raw_rows, degrees, slots), bf),
            pltpu.VMEM(spins.shape, bf),
            pltpu.VMEM((length, 2 * degrees), f32),
            pltpu.VMEM((LANES, LANES), f32),
            pltpu.VMEM((2, LANES, LANES), f32),
            pltpu.VMEM((2 * degrees, 8, LANES), f32),
            dma((fields_in,)),
            dma((fields_in,)),
            dma((fields_in,)),
            dma,
            dma,
            dma,
            dma,
            dma((2,)),
            dma((2, groups * peers)),
            dma((2, peers, groups)),
            dma((2, groups * peers)),
            dma((2, peers, groups)),
            dma((2, groups)),
        ],
        compiler_params=pltpu.CompilerParams(
            vmem_limit_bytes=VMEM_LIMIT, collective_id=0, has_side_effects=True
        ),
    )(
        maps, deltas, spins, places, mirror, order, row_cos, row_sin, row_tc, row_ts,
        col_cos, col_sin, col_tc, col_ts,
    )


def on_device(maps, deltas, spin_rows, ell_index, owner_map, prior):
    phi_count = lax.axis_size("phi")
    length = maps.shape[2] * phi_count
    peers = lax.axis_size("theta") * phi_count
    half = maps.shape[2]
    degrees = deltas.shape[1]
    slots = length // peers
    inner = length // ROW_OUTER

    residue = owner_map % ROW_OUTER
    flipped = residue > ROW_OUTER // 2
    half_map = jnp.where(flipped, length - owner_map, owner_map)
    place = lambda freq: (freq % ROW_OUTER) * inner + freq // ROW_OUTER
    places = jnp.concatenate([place(half_map), place(owner_map)])
    mirror = jnp.where(flipped, -1.0, 1.0).reshape(-1, LANES)

    k_ids = lax.axis_index("phi") * half + jnp.arange(half, dtype=jnp.int32)
    keep_rows = jnp.abs(signed(k_ids, length))[None, :] <= ell_index[:, None]
    spins = jnp.where(keep_rows[None], spin_rows.transpose(1, 2, 0), 0).reshape(2 * degrees, half)
    sums, _ = pipeline_call(peers, maps, deltas, spins, places, mirror)
    sums = sums.transpose(0, 2, 1, 3).reshape(2, degrees, 2, slots)
    scalar, spin = sums[0], sums[1]

    slot_start = (lax.axis_index("theta") * phi_count + lax.axis_index("phi")) * slots
    own_ids = lax.dynamic_slice_in_dim(owner_map, slot_start, slots)
    slot_freq = signed(own_ids, length)
    ell_float = ell_index.astype(jnp.float32)
    weight = 2.0 * math.pi / length * jnp.sqrt((2.0 * ell_float + 1.0) / (4.0 * math.pi)) / length
    keep = jnp.abs(slot_freq)[None, :] <= ell_index[:, None]
    keep_slots = keep.astype(jnp.float32) * weight[:, None]
    coupling = (prior * jnp.sqrt(ell_float * (ell_float + 1.0)) / (length // 2))[:, None]
    inner_real = (-spin[:, 1] - coupling * scalar[:, 0]) * keep_slots
    inner_imag = (spin[:, 0] - coupling * scalar[:, 1]) * keep_slots
    turns = jnp.mod(-slot_freq, 4)[None, :]
    phase_real = jnp.where(turns == 0, 1.0, jnp.where(turns == 2, -1.0, 0.0))
    phase_imag = jnp.where(turns == 1, 1.0, jnp.where(turns == 3, -1.0, 0.0))
    out_real = phase_real * inner_real - phase_imag * inner_imag
    out_imag = phase_real * inner_imag + phase_imag * inner_real
    return jnp.stack([out_real, out_imag], axis=1)


def solution(mesh):
    owner_count = mesh.shape["theta"] * mesh.shape["phi"]
    paired = mesh.shape["phi"] == 2 and owner_count in (8, 16)
    body = on_device if paired else on_device_general
    placed = (
        P("grp", "theta", "phi"),
        P("phi", None, "theta"),
        P("phi", None, None),
        P(),
        P(),
        P(),
    )
    return jax.shard_map(
        body,
        mesh=mesh,
        in_specs=placed,
        out_specs=P("grp", None, ("theta", "phi")),
        check_vma=False,
    )
```

```python
import functools
import math

import jax
import jax.numpy as jnp
import numpy as np
from jax import lax
from jax.experimental import pallas as pl
from jax.experimental.pallas import tpu as pltpu
from jax.sharding import PartitionSpec as P


def exact_einsum(form, table, operand):
    return jnp.einsum(form, table, operand, precision=lax.Precision.HIGHEST)


def angle_tables(row_count, start, count, modulus):
    freq_rows = jnp.arange(row_count, dtype=jnp.int32)
    sample_cols = start + jnp.arange(count, dtype=jnp.int32)
    angles = (
        2.0
        * math.pi
        / modulus
        * jnp.mod(freq_rows[:, None] * sample_cols[None, :], modulus).astype(jnp.float32)
    )
    return (jnp.cos(angles), jnp.sin(angles))


def row_transform(real_part, imag_part, outer_len, inner_len):
    row_count = real_part.shape[0]
    length = outer_len * inner_len
    cos_a, sin_a = angle_tables(outer_len, 0, outer_len, outer_len)
    real_blocks = real_part.reshape(row_count, outer_len, inner_len)
    section_real = exact_einsum("ka,rab->rkb", cos_a, real_blocks)
    section_imag = -exact_einsum("ka,rab->rkb", sin_a, real_blocks)
    if imag_part is not None:
        imag_blocks = imag_part.reshape(row_count, outer_len, inner_len)
        section_real = section_real + exact_einsum("ka,rab->rkb", sin_a, imag_blocks)
        section_imag = section_imag + exact_einsum("ka,rab->rkb", cos_a, imag_blocks)
    cos_t, sin_t = angle_tables(outer_len, 0, inner_len, length)
    turned_real = section_real * cos_t + section_imag * sin_t
    turned_imag = section_imag * cos_t - section_real * sin_t
    cos_b, sin_b = angle_tables(inner_len, 0, inner_len, inner_len)
    out_real = exact_einsum("qb,rkb->rqk", cos_b, turned_real) + exact_einsum(
        "qb,rkb->rqk", sin_b, turned_imag
    )
    out_imag = exact_einsum("qb,rkb->rqk", cos_b, turned_imag) - exact_einsum(
        "qb,rkb->rqk", sin_b, turned_real
    )
    return (out_real.reshape(row_count, length), out_imag.reshape(row_count, length))


def column_transform(real_part, imag_part, outer_len, inner_len, start):
    fields = real_part.shape[0]
    count = real_part.shape[2]
    slots = real_part.shape[3]
    length = outer_len * inner_len
    cos_a, sin_a = angle_tables(outer_len, 0, outer_len, outer_len)
    section_real = exact_einsum("ka,fabm->fkbm", cos_a, real_part) + exact_einsum(
        "ka,fabm->fkbm", sin_a, imag_part
    )
    section_imag = exact_einsum("ka,fabm->fkbm", cos_a, imag_part) - exact_einsum(
        "ka,fabm->fkbm", sin_a, real_part
    )
    cos_t, sin_t = angle_tables(outer_len, start, count, length)
    cos_t = cos_t[:, :, None]
    sin_t = sin_t[:, :, None]
    turned_real = section_real * cos_t + section_imag * sin_t
    turned_imag = section_imag * cos_t - section_real * sin_t
    cos_b, sin_b = angle_tables(inner_len, start, count, inner_len)
    out_real = exact_einsum("qb,fkbm->fqkm", cos_b, turned_real) + exact_einsum(
        "qb,fkbm->fqkm", sin_b, turned_imag
    )
    out_imag = exact_einsum("qb,fkbm->fqkm", cos_b, turned_imag) - exact_einsum(
        "qb,fkbm->fqkm", sin_b, turned_real
    )
    return (out_real.reshape(fields, length, slots), out_imag.reshape(fields, length, slots))


def accumulate(spectrum_block, table_block, spin_block, length, ell_index):
    count = table_block.shape[0]
    positions = jnp.arange(count, dtype=jnp.int32)
    freq = jnp.where(positions < length // 2, positions, positions - length)
    terms = []
    for degree in range(table_block.shape[1]):
        keep_rows = (jnp.abs(freq) <= ell_index[degree]).astype(jnp.float32)
        row_weights = spin_block[:, :, degree].astype(jnp.float32).T * keep_rows[None, :]
        table = table_block[:, degree, :].astype(jnp.float32)
        terms.append(
            jnp.einsum(
                "fk,ks,xfks->fxs",
                row_weights,
                table,
                spectrum_block,
                precision=lax.Precision.HIGHEST,
            )
        )
    return jnp.stack(terms)


def on_device_general(maps, deltas, spin_rows, ell_index, owner_map, prior):
    theta_count = lax.axis_size("theta")
    phi_count = lax.axis_size("phi")
    length = maps.shape[2] * phi_count
    values = maps.astype(jnp.float32)
    planes = jnp.stack([values[0], values[1] * values[2], values[1] * values[3]])
    row_planes = lax.all_to_all(planes, "phi", split_axis=1, concat_axis=2, tiled=True)
    inner_len = length // theta_count
    spectra = [
        row_transform(row_planes[0], None, theta_count, inner_len),
        row_transform(row_planes[1], row_planes[2], theta_count, inner_len),
    ]
    stacked = jnp.stack(
        [
            jnp.stack([spectrum[0] for spectrum in spectra]),
            jnp.stack([spectrum[1] for spectrum in spectra]),
        ]
    )
    permuted = jnp.take(stacked, owner_map, axis=3)
    columns = lax.all_to_all(permuted, "theta", split_axis=3, concat_axis=2, tiled=True)
    fields = columns.shape[1]
    slots = columns.shape[3]
    sub_rows = columns.shape[2] // theta_count
    blocks = columns.reshape(2, fields, theta_count, sub_rows, slots)
    row_start = lax.axis_index("phi") * sub_rows
    spec_real, spec_imag = column_transform(blocks[0], blocks[1], theta_count, inner_len, row_start)
    combined = jnp.stack([spec_real, spec_imag])
    totals = accumulate(
        combined,
        lax.all_gather(deltas, "phi", axis=0, tiled=True),
        lax.all_gather(spin_rows, "phi", axis=0, tiled=True),
        length,
        ell_index,
    )
    shares = lax.psum_scatter(totals, "phi", scatter_dimension=3, tiled=True)
    share_count = shares.shape[3]
    slot_start = lax.axis_index("theta") * slots + lax.axis_index("phi") * share_count
    share_ids = lax.dynamic_slice_in_dim(owner_map, slot_start, share_count)
    slot_freq = jnp.where(share_ids < length // 2, share_ids, share_ids - length)
    ell_float = ell_index.astype(jnp.float32)
    weight = 2.0 * math.pi / length * jnp.sqrt((2.0 * ell_float + 1.0) / (4.0 * math.pi)) / length
    keep_slots = (jnp.abs(slot_freq)[None, :] <= ell_index[:, None]).astype(jnp.float32) * weight[
        :, None
    ]
    scalar_real = shares[:, 0, 0] * keep_slots
    scalar_imag = shares[:, 0, 1] * keep_slots
    spin_real = shares[:, 1, 0] * keep_slots
    spin_imag = shares[:, 1, 1] * keep_slots
    coupling = (prior * jnp.sqrt(ell_float * (ell_float + 1.0)) / (length // 2))[:, None]
    inner_real = -spin_imag - coupling * scalar_real
    inner_imag = spin_real - coupling * scalar_imag
    turns = jnp.mod(-slot_freq, 4)
    phase_real = jnp.where(turns == 0, 1.0, jnp.where(turns == 2, -1.0, 0.0)).astype(jnp.float32)[
        None, :
    ]
    phase_imag = jnp.where(turns == 1, 1.0, jnp.where(turns == 3, -1.0, 0.0)).astype(jnp.float32)[
        None, :
    ]
    out_real = phase_real * inner_real - phase_imag * inner_imag
    out_imag = phase_real * inner_imag + phase_imag * inner_real
    return jnp.stack([out_real, out_imag], axis=1)


ROW_OUTER = 8
LANES = 128
VMEM_LIMIT = 67043328
CODE_TOP = 32767.0
MESH = pl.DeviceIdType.MESH


def cplx_add(x, y):
    return tuple(b if a is None else a if b is None else a + b for a, b in zip(x, y))


def cplx_sub(x, y):
    return tuple(
        (None if b is None else -b) if a is None else a if b is None else a - b
        for a, b in zip(x, y)
    )


def turn(x, step, count):
    real, imag = x
    if step == 0:
        return x
    if 4 * step == count:
        return (imag, None if real is None else -real)
    cos_v = math.cos(2.0 * math.pi * step / count)
    sin_v = math.sin(2.0 * math.pi * step / count)
    if imag is None:
        return (real * cos_v, real * -sin_v)
    if 8 * step == count:
        return ((real + imag) * cos_v, (imag - real) * cos_v)
    if 8 * step == 3 * count:
        return ((imag - real) * sin_v, (real + imag) * -sin_v)
    return (real * cos_v + imag * sin_v, imag * cos_v - real * sin_v)


def butterfly(items):
    count = len(items)
    if count == 1:
        return items
    even, odd = butterfly(items[::2]), butterfly(items[1::2])
    turned = [turn(x, step, count) for step, x in enumerate(odd)]
    return [cplx_add(a, b) for a, b in zip(even, turned)] + [
        cplx_sub(a, b) for a, b in zip(even, turned)
    ]


def split_store(high, low, where, value):
    top = value.astype(jnp.bfloat16)
    high[where] = top
    low[where] = (value - top.astype(jnp.float32)).astype(jnp.bfloat16)


def store_matrix(cos_v, sin_v, high, low):
    size = cos_v.shape[0]
    first, second = slice(0, size), slice(size, 2 * size)
    split_store(high, low, (first, first), cos_v)
    split_store(high, low, (first, second), sin_v)
    split_store(high, low, (second, first), -sin_v)
    split_store(high, low, (second, second), cos_v)


def dot_nt(left, right):
    return lax.dot_general(
        left, right, (((1,), (1,)), ((), ())), preferred_element_type=jnp.float32
    )


def three_dots(mat_high, mat_low, high, low):
    return dot_nt(mat_high[...], high) + dot_nt(mat_high[...], low) + dot_nt(mat_low[...], high)


def turned(item, cos_v, sin_v):
    real, imag = item
    if imag is None:
        return real * cos_v, real * -sin_v
    return real * cos_v + imag * sin_v, imag * cos_v - real * sin_v


def flip_bits(value, mask, count):
    result, bit = 0, 1
    while bit < count:
        result = result + ((value // bit + mask // bit) % 2) * bit
        bit *= 2
    return result


def pipeline_kernel(
    peers, maps, deltas, spins, owner, owner_rows, ells, priors, row_cos, row_sin, row_tc, row_ts,
    col_tc, col_ts, out_ref, land,
    planes, far_plane, x_high, x_low, row_mat_high, row_mat_low, col_mat_high, col_mat_low,
    codes, scales, stage, scale_stage, recv, scale_recv, table, raw, order, spin_land, weights,
    scale_rows, scale_cols, total, sums, plane_send, plane_recv, plane_own, far_send, far_recv,
    land_send, land_recv, spin_send, spin_recv, raw_sem, code_send, code_recv, scale_send,
    scale_sem, own_sem,
):
    theta, phi = lax.axis_index("theta"), lax.axis_index("phi")
    me = theta * 2 + phi
    other = 1 - phi
    rows = planes.shape[2]
    half = planes.shape[3]
    length = 2 * half
    inner = row_cos.shape[0]
    sub = col_tc.shape[1]
    groups = recv.shape[2]
    degrees = deltas.shape[1]
    slots = groups * LANES
    fold = rows // LANES
    near = peers // 2
    far_me = flip_bits(me, near, peers)
    parts_per_half = half // inner

    def device(index):
        return {"theta": index // 2, "phi": index % 2}

    barrier = pltpu.get_barrier_semaphore()
    for mask in range(1, peers):
        pl.semaphore_signal(
            barrier, inc=1, device_id=device(flip_bits(me, mask, peers)), device_id_type=MESH
        )
    pl.semaphore_wait(barrier, peers - 1)

    def far_copy(swap):
        target = (phi + swap) % 2
        return pltpu.make_async_remote_copy(
            src_ref=maps.at[0, pl.ds(pl.multiple_of(target * rows, rows), rows), :],
            dst_ref=far_plane.at[0, swap],
            send_sem=far_send.at[swap],
            recv_sem=far_recv.at[swap],
            device_id=device(flip_bits(me, near + swap, peers)),
            device_id_type=MESH,
        )

    def plane_copy(place):
        return pltpu.make_async_remote_copy(
            src_ref=maps.at[place, pl.ds(pl.multiple_of(other * rows, rows), rows), :],
            dst_ref=planes.at[place, 1],
            send_sem=plane_send.at[place],
            recv_sem=plane_recv.at[place],
            device_id={"phi": other},
            device_id_type=MESH,
        )

    def own_plane(place):
        return pltpu.make_async_copy(
            maps.at[place, pl.ds(pl.multiple_of(phi * rows, rows), rows), :],
            planes.at[place, 0],
            plane_own.at[place],
        )

    for swap in range(2):
        far_copy(swap).start()
    for place in range(4):
        plane_copy(place).start()
        own_plane(place).start()
    land_copy = pltpu.make_async_remote_copy(
        src_ref=deltas.at[:, :, pl.ds(pl.multiple_of(other * slots, slots), slots)],
        dst_ref=land,
        send_sem=land_send,
        recv_sem=land_recv,
        device_id={"phi": other},
        device_id_type=MESH,
    )
    land_copy.start()
    spin_copy = pltpu.make_async_remote_copy(
        src_ref=spins,
        dst_ref=spin_land,
        send_sem=spin_send,
        recv_sem=spin_recv,
        device_id={"phi": other},
        device_id_type=MESH,
    )
    spin_copy.start()
    store_matrix(row_cos[...], row_sin[...], row_mat_high, row_mat_low)

    sign = (1 - 2 * phi).astype(jnp.float32)

    def row_transform_kernel(source, places_in, kept):
        step_rows = 16

        def chunk(step, carry):
            span = pl.ds(pl.multiple_of(step * step_rows, step_rows), step_rows)
            for first in range(0, inner, LANES):

                def part(place, a):
                    start = (a % parts_per_half) * inner + first
                    return source[
                        place, a // parts_per_half, span, start : start + LANES
                    ].astype(jnp.float32)

                items = []
                for a in range(ROW_OUTER):
                    if len(places_in) == 1:
                        items.append((part(places_in[0], a), None))
                    else:
                        base = part(places_in[0], a)
                        items.append((base * part(places_in[1], a), base * part(places_in[2], a)))
                done = butterfly(items)
                for k in range(kept):
                    cos_k = row_tc[k : k + 1, first : first + LANES]
                    sin_k = row_ts[k : k + 1, first : first + LANES]
                    if k % 2:
                        cos_k, sin_k = cos_k * sign, sin_k * sign
                    real, imag = turned(done[k], cos_k, sin_k)
                    split_store(x_high, x_low, (k, span, slice(first, first + LANES)), real)
                    split_store(
                        x_high, x_low, (k, span, slice(inner + first, inner + first + LANES)), imag
                    )
            return carry

        lax.fori_loop(0, rows // step_rows, chunk, 0)

        def block(k, carry):
            both = three_dots(row_mat_high, row_mat_low, x_high[k], x_low[k])
            real, imag = both[:inner], both[inner:]
            top = jnp.max(jnp.maximum(jnp.abs(real), jnp.abs(imag)), axis=1, keepdims=True)
            top = jnp.maximum(top, 1e-30)
            factor = CODE_TOP / top
            code_real = jnp.round(real * factor).astype(jnp.int32)
            code_imag = jnp.round(imag * factor).astype(jnp.int32)
            span = pl.ds(pl.multiple_of(k * inner, inner), inner)
            codes[span, :] = (code_real << 16) | (code_imag & 0xFFFF)
            scales[span, :] = jnp.broadcast_to(top * (1.0 / CODE_TOP), (inner, LANES))
            return carry

        lax.fori_loop(0, kept, block, 0)

    def mask_of(count, n):
        if count == peers:
            return peers - 1 - n // 2 - near * (n % 2)
        return count - 1 - n

    def code_copy(field, slot, group, mask, source):
        return pltpu.make_async_remote_copy(
            src_ref=stage.at[field, slot, group],
            dst_ref=recv.at[field, source, group],
            send_sem=code_send.at[field, slot, group],
            recv_sem=code_recv.at[field, source, group],
            device_id=device(flip_bits(me, mask, peers)),
            device_id_type=MESH,
        )

    def scale_copy(field, slot, group, mask, source):
        return pltpu.make_async_remote_copy(
            src_ref=scale_stage.at[field, slot, group],
            dst_ref=scale_recv.at[field, group, source],
            send_sem=scale_send.at[field, slot, group],
            recv_sem=scale_sem.at[field, source, group],
            device_id=device(flip_bits(me, mask, peers)),
            device_id_type=MESH,
        )

    def own_copy(field, slot, group, source, which):
        return pltpu.make_async_copy(
            stage.at[field, slot, group], recv.at[field, source, group], own_sem.at[which, group]
        )

    lane = lax.broadcasted_iota(jnp.int32, (1, LANES), 1)
    unroll = 8
    shift = ROW_OUTER.bit_length() - 1

    def send_block(field, base, count, group, n, source, which):
        @pl.when(n != count - 1)
        def _():
            mask = mask_of(count, n)
            code_copy(field, base + n, group, mask, source).start()
            scale_copy(field, base + n, group, mask, source).start()

        @pl.when(n == count - 1)
        def _():
            own_copy(field, base + n, group, source, which).start()

    def gather_blocks(field, base, count, first_group, last_group, source, which, send):
        def step_body(step, carry):
            group, n = step // count, step % count
            dest = flip_bits(me, mask_of(count, n), peers)
            first = dest * slots + group * LANES

            def rows_body(g, acc):
                start = pl.multiple_of(g * unroll, unroll)
                for u in range(unroll):
                    freq = owner[first + start + u]
                    if field == 0:
                        mirrored = (freq & (ROW_OUTER - 1)) > ROW_OUTER // 2
                        freq = jnp.where(mirrored, length - freq, freq)
                    where = (freq & (ROW_OUTER - 1)) * inner + (freq >> shift)
                    stage[field, base + n, group, pl.ds(start + u, 1), :] = codes[
                        pl.ds(where, 1), :
                    ]
                    acc = jnp.where(lane == start + u, scales[pl.ds(where, 1), :], acc)
                return acc

            acc = lax.fori_loop(0, LANES // unroll, rows_body, jnp.zeros((1, LANES), jnp.float32))
            scale_stage[field, base + n, group] = acc

            if send:

                @pl.when(step > first_group * count)
                def _():
                    before = step - 1
                    send_block(field, base, count, before // count, before % count, source, which)

            return carry

        lax.fori_loop(first_group * count, last_group * count, step_body, 0)
        if send:
            send_block(field, base, count, last_group - 1, count - 1, source, which)

    own_plane(0).wait()
    plane_copy(0).wait_recv()
    row_transform_kernel(planes, (0,), ROW_OUTER // 2 + 1)
    gather_blocks(0, 0, near, 0, groups, me, 0, True)
    for place in range(1, 4):
        own_plane(place).wait()
        plane_copy(place).wait_recv()
    row_transform_kernel(planes, (1, 2, 3), ROW_OUTER)
    gather_blocks(1, 0, peers, 0, groups - 1, me, 2, True)
    gather_blocks(1, 0, peers, groups - 1, groups, me, 2, False)

    for swap in range(2):
        far_copy(swap).wait_recv()
    row_transform_kernel(far_plane, (0,), ROW_OUTER // 2 + 1)
    gather_blocks(0, near, near, 0, groups, far_me, 1, True)

    def send_last(n, carry):
        send_block(1, 0, peers, groups - 1, n, me, 2)
        return carry

    lax.fori_loop(0, peers, send_last, 0)

    skip = inner // sub
    thinned = []
    for index, wave in enumerate((row_cos, row_sin)):
        for first in range(0, sub, LANES):
            start = index * inner * (sub // LANES) + first // LANES * inner
            scales[start : start + inner, :] = wave[:, first : first + LANES]
        thinned.append(
            jnp.concatenate(
                [
                    scales[
                        pl.ds(index * inner * (sub // LANES) + first // LANES * inner, sub, skip), :
                    ]
                    for first in range(0, sub, LANES)
                ],
                axis=1,
            )
        )
    store_matrix(*thinned, col_mat_high, col_mat_low)
    spin_copy.wait_recv()
    eye_row = lax.broadcasted_iota(jnp.int32, (LANES, LANES), 0)
    eye_col = lax.broadcasted_iota(jnp.int32, (LANES, LANES), 1)
    eye = (eye_row == eye_col).astype(jnp.float32).astype(jnp.bfloat16)
    column = lax.broadcasted_iota(jnp.int32, (1, degrees), 1)
    bound = jnp.zeros((1, degrees), jnp.int32)
    for j in range(degrees):
        bound = jnp.where(column == j, ells[j], bound)
    for which, ref in ((phi, spins), (other, spin_land)):
        for first in range(0, half, LANES):
            start = pl.multiple_of(which * half + first, LANES)
            span = pl.ds(start, LANES)
            k_id = lax.broadcasted_iota(jnp.int32, (LANES, 1), 0) + start
            keep = jnp.abs(signed(k_id, length)) <= bound
            for spin in range(2):
                value = dot_nt(eye, ref[spin, :, first : first + LANES])
                weights[span, spin * degrees : (spin + 1) * degrees] = jnp.where(keep, value, 0.0)

    raw_rows = raw.shape[1]
    raw_q = raw_rows // peers
    raw_steps = half // raw_rows
    small = raw_q // 2
    width = small * peers * degrees
    target = lax.broadcasted_iota(jnp.int32, (width, width), 0)
    source_row = lax.broadcasted_iota(jnp.int32, (width, width), 1)
    polar, degree_id = source_row // degrees, source_row % degrees
    wanted = (polar % peers * degrees + degree_id) * small + polar // peers
    order[...] = (wanted == target).astype(jnp.float32).astype(jnp.bfloat16)

    def raw_copy(ref, lanes, step):
        return pltpu.make_async_copy(
            ref.at[pl.ds(pl.multiple_of(step * raw_rows, raw_rows), raw_rows), :, lanes],
            raw.at[step % 2],
            raw_sem.at[step % 2],
        )

    def reorder(ref, lanes, which):
        raw_copy(ref, lanes, 0).start()

        def body(step, carry):
            @pl.when(step + 1 < raw_steps)
            def _():
                raw_copy(ref, lanes, step + 1).start()

            raw_copy(ref, lanes, step).wait()
            base = pl.multiple_of(which * (sub // 2) + step * raw_q, raw_q)
            for group in range(groups):
                pieces = []
                for top in range(0, raw_rows, raw_rows // 2):
                    source = raw[
                        step % 2, top : top + raw_rows // 2, :, group * LANES : (group + 1) * LANES
                    ].reshape(raw_rows // 2 * degrees, LANES)
                    pieces.append(
                        jnp.dot(order[...], source, preferred_element_type=jnp.float32)
                    )
                for k in range(peers):
                    for j in range(degrees):
                        start = (k * degrees + j) * small
                        table[group, k, j, pl.ds(base, raw_q), :] = jnp.concatenate(
                            [piece[start : start + small] for piece in pieces], axis=0
                        ).astype(jnp.bfloat16)
            return carry

        lax.fori_loop(0, raw_steps, body, 0)

    reorder(deltas, pl.ds(pl.multiple_of(phi * slots, slots), slots), phi)
    land_copy.wait_recv()
    reorder(land, pl.ds(0, slots), other)

    scale_rows[...] = jnp.zeros_like(scale_rows)

    def column_block(position, carry):
        early = position < groups - 1
        scalar_turn = (position >= groups - 1) & (position < 2 * groups - 1)
        field = jnp.where(scalar_turn, 0, 1)
        group = jnp.where(
            early, position, jnp.where(scalar_turn, position - (groups - 1), groups - 1)
        )

        @pl.when(field == 0)
        def _():
            def wait_one(n, inner_carry):
                mask = mask_of(near, n)
                peer = flip_bits(me, mask, peers)
                code_copy(0, n, group, mask, peer).wait_recv()
                scale_copy(0, n, group, mask, peer).wait_recv()
                across = flip_bits(peer, near, peers)
                code_copy(0, near + n, group, mask, across).wait_recv()
                scale_copy(0, near + n, group, mask, across).wait_recv()
                return inner_carry

            lax.fori_loop(0, near - 1, wait_one, 0)
            own_copy(0, near - 1, group, me, 0).wait()
            own_copy(0, 2 * near - 1, group, far_me, 1).wait()
            scale_recv[0, group, me] = scale_stage[0, near - 1, group]
            scale_recv[0, group, far_me] = scale_stage[0, 2 * near - 1, group]

        @pl.when(field == 1)
        def _():
            def wait_one(n, inner_carry):
                mask = mask_of(peers, n)
                peer = flip_bits(me, mask, peers)
                code_copy(1, n, group, mask, peer).wait_recv()
                scale_copy(1, n, group, mask, peer).wait_recv()
                return inner_carry

            lax.fori_loop(0, peers - 1, wait_one, 0)
            own_copy(1, peers - 1, group, me, 2).wait()
            scale_recv[1, group, me] = scale_stage[1, peers - 1, group]

        for a in range(peers):
            scale_rows[a : a + 1, :] = scale_recv[field, group, a]
        plain = scale_rows[...]
        own_freq = owner_rows[pl.ds(me * groups + group, 1), :]
        mirrored = ((own_freq & (ROW_OUTER - 1)) > ROW_OUTER // 2) & (field == 0)
        scale_cols[0] = plain.T
        scale_cols[1] = jnp.where(mirrored, -plain, plain).T
        step_rows = 16

        def chunk(step, inner_carry):
            span = pl.ds(pl.multiple_of(step * step_rows, step_rows), step_rows)
            sre, sim = scale_cols[0, span, :], scale_cols[1, span, :]
            for first in range(0, sub, LANES):
                items = []
                for a in range(peers):
                    code = recv[field, a, group, span, first : first + LANES]
                    real = (code >> 16).astype(jnp.float32) * sre[:, a : a + 1]
                    imag = ((code << 16) >> 16).astype(jnp.float32) * sim[:, a : a + 1]
                    items.append((real, imag))
                for k, item in enumerate(butterfly(items)):
                    real, imag = turned(
                        item,
                        col_tc[k : k + 1, first : first + LANES],
                        col_ts[k : k + 1, first : first + LANES],
                    )
                    start = pl.multiple_of(k % fold * LANES + step * step_rows, step_rows)
                    place = pl.ds(start, step_rows)
                    split_store(
                        x_high, x_low, (k // fold, place, slice(first, first + LANES)), real
                    )
                    split_store(
                        x_high, x_low,
                        (k // fold, place, slice(sub + first, sub + first + LANES)), imag,
                    )
            return inner_carry

        lax.fori_loop(0, LANES // step_rows, chunk, 0)
        total[...] = jnp.zeros_like(total)

        def block(k2, inner_carry):
            where = (k2, slice(0, rows), slice(0, 2 * sub))
            both = three_dots(col_mat_high, col_mat_low, x_high[where], x_low[where])
            for r in range(fold):
                k = k2 * fold + r
                span = slice(r * LANES, (r + 1) * LANES)
                real, imag = both[:sub, span], both[sub:, span]
                eight = weights[pl.ds(k, sub, peers), :]
                four = jnp.where(field == 0, eight[:, :degrees], eight[:, degrees : 2 * degrees])
                for j in range(degrees):
                    weighted = table[group, k, j].astype(jnp.float32) * four[:, j : j + 1]
                    for part, value in enumerate((real, imag)):
                        total[2 * j + part] += jnp.sum(
                            (weighted * value).reshape(sub // 8, 8, LANES), axis=0
                        )
            return inner_carry

        lax.fori_loop(0, peers // fold, block, 0)
        sums[field, group] = jnp.sum(total[...], axis=1)
        return carry

    lax.fori_loop(0, 2 * groups, column_block, 0)

    for group in range(groups):
        slot_freq = signed(owner_rows[pl.ds(me * groups + group, 1), :], length)
        turns = -slot_freq & 3
        phase_real = jnp.where(turns == 0, 1.0, jnp.where(turns == 2, -1.0, 0.0))
        phase_imag = jnp.where(turns == 1, 1.0, jnp.where(turns == 3, -1.0, 0.0))
        scalar, spin = sums[0, group], sums[1, group]
        for j in range(degrees):
            ell = jnp.full((1, LANES), ells[j], jnp.int32)
            ell_float = ell.astype(jnp.float32)
            weight = jnp.sqrt((2.0 * ell_float + 1.0) / (4.0 * math.pi))
            weight = weight * (2.0 * math.pi / length / length)
            keep = jnp.where(jnp.abs(slot_freq) <= ell, weight, 0.0)
            coupling = priors[j] * jnp.sqrt(ell_float * (ell_float + 1.0)) * (2.0 / length)
            re, im = 2 * j, 2 * j + 1
            inner_real = (-spin[im : im + 1] - coupling * scalar[re : re + 1]) * keep
            inner_imag = (spin[re : re + 1] - coupling * scalar[im : im + 1]) * keep
            span = slice(group * LANES, (group + 1) * LANES)
            out_ref[j, 0:1, span] = phase_real * inner_real - phase_imag * inner_imag
            out_ref[j, 1:2, span] = phase_real * inner_imag + phase_imag * inner_real

    for place in range(4):
        plane_copy(place).wait_send()
    for swap in range(2):
        far_copy(swap).wait_send()
    land_copy.wait_send()
    spin_copy.wait_send()

    def finish(count):
        def body(n, carry):
            for group in range(groups):
                for field, base in ((0, 0), (0, near)) if count == near else ((1, 0),):
                    mask = mask_of(count, n)
                    code_copy(field, base + n, group, mask, me).wait_send()
                    scale_copy(field, base + n, group, mask, me).wait_send()
            return carry

        lax.fori_loop(0, count - 1, body, 0)

    finish(near)
    finish(peers)


def wave_tables(row_ids, col_ids, modulus):
    angles = 2.0 * math.pi / modulus * ((row_ids[:, None] * col_ids[None, :]) % modulus)
    return np.cos(angles).astype(np.float32), np.sin(angles).astype(np.float32)


def signed(ids, length):
    return jnp.where(ids < length // 2, ids, ids - length)


def pipeline_call(peers, maps, deltas, spins, owner_map, ell_index, prior):
    fields_in, rows_all, half = maps.shape
    rows = rows_all // 2
    length = 2 * half
    slots = deltas.shape[2] // 2
    degrees = deltas.shape[1]
    groups = slots // LANES
    inner = length // ROW_OUTER
    sub = length // peers
    ids = np.arange(length)
    row_cos, row_sin = wave_tables(ids[:inner], ids[:inner], inner)
    row_tc, row_ts = wave_tables(ids[:ROW_OUTER], ids[:inner], length)
    col_tc, col_ts = wave_tables(ids[:peers], ids[:sub], length)
    small = 8
    raw_rows = 2 * small * peers
    width = small * peers * degrees
    bf, f32 = jnp.bfloat16, jnp.float32
    vmem = pl.BlockSpec(memory_space=pltpu.VMEM)
    smem = pl.BlockSpec(memory_space=pltpu.SMEM)
    anywhere = pl.BlockSpec(memory_space=pl.ANY)
    dma = pltpu.SemaphoreType.DMA
    return pl.pallas_call(
        functools.partial(pipeline_kernel, peers),
        in_specs=[anywhere, anywhere, vmem, smem, vmem, smem, smem] + [vmem] * 6,
        out_specs=[vmem, anywhere],
        out_shape=[
            jax.ShapeDtypeStruct((degrees, 2, slots), f32),
            jax.ShapeDtypeStruct((half, degrees, slots), bf),
        ],
        scratch_shapes=[
            pltpu.VMEM((fields_in, 2, rows, half), bf),
            pltpu.VMEM((1, 2, rows, half), bf),
            pltpu.VMEM((ROW_OUTER, rows, 2 * inner), bf),
            pltpu.VMEM((ROW_OUTER, rows, 2 * inner), bf),
            pltpu.VMEM((2 * inner, 2 * inner), bf),
            pltpu.VMEM((2 * inner, 2 * inner), bf),
            pltpu.VMEM((2 * sub, 2 * sub), bf),
            pltpu.VMEM((2 * sub, 2 * sub), bf),
            pltpu.VMEM((length, rows), jnp.int32),
            pltpu.VMEM((length, LANES), f32),
            pltpu.VMEM((2, peers, groups, LANES, rows), jnp.int32),
            pltpu.VMEM((2, peers, groups, 1, LANES), f32),
            pltpu.VMEM((2, peers, groups, LANES, rows), jnp.int32),
            pltpu.VMEM((2, groups, peers, 1, LANES), f32),
            pltpu.VMEM((groups, peers, degrees, sub, LANES), bf),
            pltpu.VMEM((2, raw_rows, degrees, slots), bf),
            pltpu.VMEM((width, width), bf),
            pltpu.VMEM(spins.shape, bf),
            pltpu.VMEM((length, 2 * degrees), f32),
            pltpu.VMEM((LANES, LANES), f32),
            pltpu.VMEM((2, LANES, LANES), f32),
            pltpu.VMEM((2 * degrees, 8, LANES), f32),
            pltpu.VMEM((2, groups, 2 * degrees, LANES), f32),
            dma((fields_in,)),
            dma((fields_in,)),
            dma((fields_in,)),
            dma((2,)),
            dma((2,)),
            dma,
            dma,
            dma,
            dma,
            dma((2,)),
            dma((2, peers, groups)),
            dma((2, peers, groups)),
            dma((2, peers, groups)),
            dma((2, peers, groups)),
            dma((3, groups)),
        ],
        compiler_params=pltpu.CompilerParams(
            vmem_limit_bytes=VMEM_LIMIT, collective_id=0, has_side_effects=True
        ),
    )(
        maps, deltas, spins, owner_map, owner_map.reshape(-1, LANES), ell_index, prior,
        row_cos, row_sin, row_tc, row_ts, col_tc, col_ts,
    )[0]


def on_device(maps, deltas, spin_rows, ell_index, owner_map, prior):
    peers = lax.axis_size("theta") * lax.axis_size("phi")
    spins = spin_rows.transpose(1, 2, 0)
    return pipeline_call(peers, maps, deltas, spins, owner_map, ell_index, prior)


def solution(mesh):
    owner_count = mesh.shape["theta"] * mesh.shape["phi"]
    paired = mesh.shape["phi"] == 2 and owner_count == 16
    body = on_device if paired else on_device_general
    placed = (
        P("grp", "theta", "phi"),
        P("phi", None, "theta"),
        P("phi", None, None),
        P(),
        P(),
        P(),
    )
    return jax.shard_map(
        body,
        mesh=mesh,
        in_specs=placed,
        out_specs=P("grp", None, ("theta", "phi")),
        check_vma=False,
    )
```

```python
import functools
import math

import jax
import jax.numpy as jnp
import numpy as np
from jax import lax
from jax.experimental import pallas as pl
from jax.experimental.pallas import tpu as pltpu
from jax.sharding import PartitionSpec as P


def exact_einsum(form, table, operand):
    return jnp.einsum(form, table, operand, precision=lax.Precision.HIGHEST)


def angle_tables(row_count, start, count, modulus):
    freq_rows = jnp.arange(row_count, dtype=jnp.int32)
    sample_cols = start + jnp.arange(count, dtype=jnp.int32)
    angles = (
        2.0
        * math.pi
        / modulus
        * jnp.mod(freq_rows[:, None] * sample_cols[None, :], modulus).astype(jnp.float32)
    )
    return (jnp.cos(angles), jnp.sin(angles))


def row_transform(real_part, imag_part, outer_len, inner_len):
    row_count = real_part.shape[0]
    length = outer_len * inner_len
    cos_a, sin_a = angle_tables(outer_len, 0, outer_len, outer_len)
    real_blocks = real_part.reshape(row_count, outer_len, inner_len)
    section_real = exact_einsum("ka,rab->rkb", cos_a, real_blocks)
    section_imag = -exact_einsum("ka,rab->rkb", sin_a, real_blocks)
    if imag_part is not None:
        imag_blocks = imag_part.reshape(row_count, outer_len, inner_len)
        section_real = section_real + exact_einsum("ka,rab->rkb", sin_a, imag_blocks)
        section_imag = section_imag + exact_einsum("ka,rab->rkb", cos_a, imag_blocks)
    cos_t, sin_t = angle_tables(outer_len, 0, inner_len, length)
    turned_real = section_real * cos_t + section_imag * sin_t
    turned_imag = section_imag * cos_t - section_real * sin_t
    cos_b, sin_b = angle_tables(inner_len, 0, inner_len, inner_len)
    out_real = exact_einsum("qb,rkb->rqk", cos_b, turned_real) + exact_einsum(
        "qb,rkb->rqk", sin_b, turned_imag
    )
    out_imag = exact_einsum("qb,rkb->rqk", cos_b, turned_imag) - exact_einsum(
        "qb,rkb->rqk", sin_b, turned_real
    )
    return (out_real.reshape(row_count, length), out_imag.reshape(row_count, length))


def column_transform(real_part, imag_part, outer_len, inner_len, start):
    fields = real_part.shape[0]
    count = real_part.shape[2]
    slots = real_part.shape[3]
    length = outer_len * inner_len
    cos_a, sin_a = angle_tables(outer_len, 0, outer_len, outer_len)
    section_real = exact_einsum("ka,fabm->fkbm", cos_a, real_part) + exact_einsum(
        "ka,fabm->fkbm", sin_a, imag_part
    )
    section_imag = exact_einsum("ka,fabm->fkbm", cos_a, imag_part) - exact_einsum(
        "ka,fabm->fkbm", sin_a, real_part
    )
    cos_t, sin_t = angle_tables(outer_len, start, count, length)
    cos_t = cos_t[:, :, None]
    sin_t = sin_t[:, :, None]
    turned_real = section_real * cos_t + section_imag * sin_t
    turned_imag = section_imag * cos_t - section_real * sin_t
    cos_b, sin_b = angle_tables(inner_len, start, count, inner_len)
    out_real = exact_einsum("qb,fkbm->fqkm", cos_b, turned_real) + exact_einsum(
        "qb,fkbm->fqkm", sin_b, turned_imag
    )
    out_imag = exact_einsum("qb,fkbm->fqkm", cos_b, turned_imag) - exact_einsum(
        "qb,fkbm->fqkm", sin_b, turned_real
    )
    return (out_real.reshape(fields, length, slots), out_imag.reshape(fields, length, slots))


def accumulate(spectrum_block, table_block, spin_block, length, ell_index):
    count = table_block.shape[0]
    positions = jnp.arange(count, dtype=jnp.int32)
    freq = jnp.where(positions < length // 2, positions, positions - length)
    terms = []
    for degree in range(table_block.shape[1]):
        keep_rows = (jnp.abs(freq) <= ell_index[degree]).astype(jnp.float32)
        row_weights = spin_block[:, :, degree].astype(jnp.float32).T * keep_rows[None, :]
        table = table_block[:, degree, :].astype(jnp.float32)
        terms.append(
            jnp.einsum(
                "fk,ks,xfks->fxs",
                row_weights,
                table,
                spectrum_block,
                precision=lax.Precision.HIGHEST,
            )
        )
    return jnp.stack(terms)


def on_device_general(maps, deltas, spin_rows, ell_index, owner_map, prior):
    theta_count = lax.axis_size("theta")
    phi_count = lax.axis_size("phi")
    length = maps.shape[2] * phi_count
    values = maps.astype(jnp.float32)
    planes = jnp.stack([values[0], values[1] * values[2], values[1] * values[3]])
    row_planes = lax.all_to_all(planes, "phi", split_axis=1, concat_axis=2, tiled=True)
    inner_len = length // theta_count
    spectra = [
        row_transform(row_planes[0], None, theta_count, inner_len),
        row_transform(row_planes[1], row_planes[2], theta_count, inner_len),
    ]
    stacked = jnp.stack(
        [
            jnp.stack([spectrum[0] for spectrum in spectra]),
            jnp.stack([spectrum[1] for spectrum in spectra]),
        ]
    )
    permuted = jnp.take(stacked, owner_map, axis=3)
    columns = lax.all_to_all(permuted, "theta", split_axis=3, concat_axis=2, tiled=True)
    fields = columns.shape[1]
    slots = columns.shape[3]
    sub_rows = columns.shape[2] // theta_count
    blocks = columns.reshape(2, fields, theta_count, sub_rows, slots)
    row_start = lax.axis_index("phi") * sub_rows
    spec_real, spec_imag = column_transform(blocks[0], blocks[1], theta_count, inner_len, row_start)
    combined = jnp.stack([spec_real, spec_imag])
    totals = accumulate(
        combined,
        lax.all_gather(deltas, "phi", axis=0, tiled=True),
        lax.all_gather(spin_rows, "phi", axis=0, tiled=True),
        length,
        ell_index,
    )
    shares = lax.psum_scatter(totals, "phi", scatter_dimension=3, tiled=True)
    share_count = shares.shape[3]
    slot_start = lax.axis_index("theta") * slots + lax.axis_index("phi") * share_count
    share_ids = lax.dynamic_slice_in_dim(owner_map, slot_start, share_count)
    slot_freq = jnp.where(share_ids < length // 2, share_ids, share_ids - length)
    ell_float = ell_index.astype(jnp.float32)
    weight = 2.0 * math.pi / length * jnp.sqrt((2.0 * ell_float + 1.0) / (4.0 * math.pi)) / length
    keep_slots = (jnp.abs(slot_freq)[None, :] <= ell_index[:, None]).astype(jnp.float32) * weight[
        :, None
    ]
    scalar_real = shares[:, 0, 0] * keep_slots
    scalar_imag = shares[:, 0, 1] * keep_slots
    spin_real = shares[:, 1, 0] * keep_slots
    spin_imag = shares[:, 1, 1] * keep_slots
    coupling = (prior * jnp.sqrt(ell_float * (ell_float + 1.0)) / (length // 2))[:, None]
    inner_real = -spin_imag - coupling * scalar_real
    inner_imag = spin_real - coupling * scalar_imag
    turns = jnp.mod(-slot_freq, 4)
    phase_real = jnp.where(turns == 0, 1.0, jnp.where(turns == 2, -1.0, 0.0)).astype(jnp.float32)[
        None, :
    ]
    phase_imag = jnp.where(turns == 1, 1.0, jnp.where(turns == 3, -1.0, 0.0)).astype(jnp.float32)[
        None, :
    ]
    out_real = phase_real * inner_real - phase_imag * inner_imag
    out_imag = phase_real * inner_imag + phase_imag * inner_real
    return jnp.stack([out_real, out_imag], axis=1)


ROW_OUTER = 8
LANES = 128
BLOCK = 64
VMEM_LIMIT = 67043328
CODE_TOP = 32767.0
MESH = pl.DeviceIdType.MESH


def cplx_add(x, y):
    return tuple(b if a is None else a if b is None else a + b for a, b in zip(x, y))


def cplx_sub(x, y):
    return tuple(
        (None if b is None else -b) if a is None else a if b is None else a - b
        for a, b in zip(x, y)
    )


def turn(x, step, count):
    real, imag = x
    if step == 0:
        return x
    if 4 * step == count:
        return (imag, None if real is None else -real)
    cos_v = math.cos(2.0 * math.pi * step / count)
    sin_v = math.sin(2.0 * math.pi * step / count)
    if imag is None:
        return (real * cos_v, real * -sin_v)
    if 8 * step == count:
        return ((real + imag) * cos_v, (imag - real) * cos_v)
    if 8 * step == 3 * count:
        return ((imag - real) * sin_v, (real + imag) * -sin_v)
    return (real * cos_v + imag * sin_v, imag * cos_v - real * sin_v)


def butterfly(items):
    count = len(items)
    if count == 1:
        return items
    even, odd = butterfly(items[::2]), butterfly(items[1::2])
    turned = [turn(x, step, count) for step, x in enumerate(odd)]
    return [cplx_add(a, b) for a, b in zip(even, turned)] + [
        cplx_sub(a, b) for a, b in zip(even, turned)
    ]


def split_store(high, low, where, value):
    top = value.astype(jnp.bfloat16)
    high[where] = top
    low[where] = (value - top.astype(jnp.float32)).astype(jnp.bfloat16)


def store_matrix(cos_v, sin_v, high, low):
    size = cos_v.shape[0]
    first, second = slice(0, size), slice(size, 2 * size)
    split_store(high, low, (first, first), cos_v)
    split_store(high, low, (first, second), sin_v)
    split_store(high, low, (second, first), -sin_v)
    split_store(high, low, (second, second), cos_v)


def dot_nt(left, right):
    return lax.dot_general(
        left, right, (((1,), (1,)), ((), ())), preferred_element_type=jnp.float32
    )


def three_dots(mat_high, mat_low, high, low):
    return dot_nt(mat_high[...], high) + dot_nt(mat_high[...], low) + dot_nt(mat_low[...], high)


def turned(item, cos_v, sin_v):
    real, imag = item
    if imag is None:
        return real * cos_v, real * -sin_v
    return real * cos_v + imag * sin_v, imag * cos_v - real * sin_v


def flip_bits(value, mask, count):
    result, bit = 0, 1
    while bit < count:
        result = result + ((value // bit + mask // bit) % 2) * bit
        bit *= 2
    return result


def pipeline_kernel(
    peers, maps, deltas, spins, owner, owner_rows, ells, priors, row_cos, row_sin, row_tc, row_ts,
    col_tc, col_ts, out_ref, land,
    planes, far_plane, x_high, x_low, row_mat_high, row_mat_low, col_mat_high, col_mat_low,
    codes, scales, stage, scale_stage, recv, scale_recv, table, raw, order, spin_land, weights,
    scale_rows, scale_cols, total, sums, plane_send, plane_recv, plane_own, far_send, far_recv,
    land_send, land_recv, spin_send, spin_recv, raw_sem, code_send, code_recv, scale_send,
    scale_sem, own_sem,
):
    theta, phi = lax.axis_index("theta"), lax.axis_index("phi")
    me = theta * 2 + phi
    other = 1 - phi
    rows = planes.shape[2]
    half = planes.shape[3]
    length = 2 * half
    inner = row_cos.shape[0]
    sub = col_tc.shape[1]
    groups = recv.shape[2]
    degrees = deltas.shape[1]
    slots = groups * BLOCK
    fold = rows // BLOCK
    early = 1
    split = LANES // BLOCK
    near = peers // 2
    far_me = flip_bits(me, near, peers)
    parts_per_half = half // inner

    def device(index):
        return {"theta": index // 2, "phi": index % 2}

    barrier = pltpu.get_barrier_semaphore()
    for mask in range(1, peers):
        pl.semaphore_signal(
            barrier, inc=1, device_id=device(flip_bits(me, mask, peers)), device_id_type=MESH
        )
    pl.semaphore_wait(barrier, peers - 1)

    def far_copy(swap):
        target = (phi + swap) % 2
        return pltpu.make_async_remote_copy(
            src_ref=maps.at[0, pl.ds(pl.multiple_of(target * rows, rows), rows), :],
            dst_ref=far_plane.at[0, swap],
            send_sem=far_send.at[swap],
            recv_sem=far_recv.at[swap],
            device_id=device(flip_bits(me, near + swap, peers)),
            device_id_type=MESH,
        )

    def plane_copy(place):
        return pltpu.make_async_remote_copy(
            src_ref=maps.at[place, pl.ds(pl.multiple_of(other * rows, rows), rows), :],
            dst_ref=planes.at[place, 1],
            send_sem=plane_send.at[place],
            recv_sem=plane_recv.at[place],
            device_id={"phi": other},
            device_id_type=MESH,
        )

    def own_plane(place):
        return pltpu.make_async_copy(
            maps.at[place, pl.ds(pl.multiple_of(phi * rows, rows), rows), :],
            planes.at[place, 0],
            plane_own.at[place],
        )

    for swap in range(2):
        far_copy(swap).start()
    for place in range(4):
        plane_copy(place).start()
        own_plane(place).start()
    land_copy = pltpu.make_async_remote_copy(
        src_ref=deltas.at[:, :, pl.ds(pl.multiple_of(other * slots, slots), slots)],
        dst_ref=land,
        send_sem=land_send,
        recv_sem=land_recv,
        device_id={"phi": other},
        device_id_type=MESH,
    )
    land_copy.start()
    spin_copy = pltpu.make_async_remote_copy(
        src_ref=spins,
        dst_ref=spin_land,
        send_sem=spin_send,
        recv_sem=spin_recv,
        device_id={"phi": other},
        device_id_type=MESH,
    )
    spin_copy.start()
    store_matrix(row_cos[...], row_sin[...], row_mat_high, row_mat_low)

    sign = (1 - 2 * phi).astype(jnp.float32)

    def row_transform_kernel(source, places_in, kept):
        step_rows = 16

        def chunk(step, carry):
            span = pl.ds(pl.multiple_of(step * step_rows, step_rows), step_rows)
            for first in range(0, inner, LANES):

                def part(place, a):
                    start = (a % parts_per_half) * inner + first
                    return source[
                        place, a // parts_per_half, span, start : start + LANES
                    ].astype(jnp.float32)

                items = []
                for a in range(ROW_OUTER):
                    if len(places_in) == 1:
                        items.append((part(places_in[0], a), None))
                    else:
                        base = part(places_in[0], a)
                        items.append((base * part(places_in[1], a), base * part(places_in[2], a)))
                done = butterfly(items)
                for k in range(kept):
                    cos_k = row_tc[k : k + 1, first : first + LANES]
                    sin_k = row_ts[k : k + 1, first : first + LANES]
                    if k % 2:
                        cos_k, sin_k = cos_k * sign, sin_k * sign
                    real, imag = turned(done[k], cos_k, sin_k)
                    split_store(x_high, x_low, (k, span, slice(first, first + LANES)), real)
                    split_store(
                        x_high, x_low, (k, span, slice(inner + first, inner + first + LANES)), imag
                    )
            return carry

        lax.fori_loop(0, rows // step_rows, chunk, 0)

        def block(k, carry):
            both = three_dots(row_mat_high, row_mat_low, x_high[k], x_low[k])
            real, imag = both[:inner], both[inner:]
            top = jnp.max(jnp.maximum(jnp.abs(real), jnp.abs(imag)), axis=1, keepdims=True)
            top = jnp.maximum(top, 1e-30)
            factor = CODE_TOP / top
            code_real = jnp.round(real * factor).astype(jnp.int32)
            code_imag = jnp.round(imag * factor).astype(jnp.int32)
            span = pl.ds(pl.multiple_of(k * inner, inner), inner)
            codes[span, :] = (code_real << 16) | (code_imag & 0xFFFF)
            scales[span, :] = jnp.broadcast_to(top * (1.0 / CODE_TOP), (inner, LANES))
            return carry

        lax.fori_loop(0, kept, block, 0)

    def mask_of(count, n):
        if count == peers:
            return peers - 1 - n // 2 - near * (n % 2)
        return count - 1 - n

    def code_copy(field, slot, group, mask, source):
        return pltpu.make_async_remote_copy(
            src_ref=stage.at[field, slot, group],
            dst_ref=recv.at[field, source, group],
            send_sem=code_send.at[field, slot, group],
            recv_sem=code_recv.at[field, source, group],
            device_id=device(flip_bits(me, mask, peers)),
            device_id_type=MESH,
        )

    def scale_copy(field, slot, group, mask, source):
        return pltpu.make_async_remote_copy(
            src_ref=scale_stage.at[field, slot, group],
            dst_ref=scale_recv.at[field, group, source],
            send_sem=scale_send.at[field, slot, group],
            recv_sem=scale_sem.at[field, source, group],
            device_id=device(flip_bits(me, mask, peers)),
            device_id_type=MESH,
        )

    def own_copy(field, slot, group, source, which):
        return pltpu.make_async_copy(
            stage.at[field, slot, group], recv.at[field, source, group], own_sem.at[which, group]
        )

    lane = lax.broadcasted_iota(jnp.int32, (1, LANES), 1)
    unroll = 8
    shift = ROW_OUTER.bit_length() - 1

    def send_block(field, base, count, group, n, source, which):
        @pl.when(n != count - 1)
        def _():
            mask = mask_of(count, n)
            code_copy(field, base + n, group, mask, source).start()
            scale_copy(field, base + n, group, mask, source).start()

        @pl.when(n == count - 1)
        def _():
            own_copy(field, base + n, group, source, which).start()

    def gather_blocks(field, base, count, source, which, sent_groups):
        def step_body(step, carry):
            group, n = step // count, step % count
            dest = flip_bits(me, mask_of(count, n), peers)
            first = dest * slots + group * BLOCK
            shown = lane - group % split * BLOCK

            def rows_body(g, acc):
                start = pl.multiple_of(g * unroll, unroll)
                for u in range(unroll):
                    freq = owner[first + start + u]
                    if field == 0:
                        mirrored = (freq & (ROW_OUTER - 1)) > ROW_OUTER // 2
                        freq = jnp.where(mirrored, length - freq, freq)
                    where = (freq & (ROW_OUTER - 1)) * inner + (freq >> shift)
                    stage[field, base + n, group, pl.ds(start + u, 1), :] = codes[
                        pl.ds(where, 1), :
                    ]
                    acc = jnp.where(shown == start + u, scales[pl.ds(where, 1), :], acc)
                return acc

            acc = lax.fori_loop(0, BLOCK // unroll, rows_body, jnp.zeros((1, LANES), jnp.float32))
            scale_stage[field, base + n, group] = acc

            @pl.when((step > 0) & (step <= sent_groups * count))
            def _():
                before = step - 1
                send_block(field, base, count, before // count, before % count, source, which)

            return carry

        lax.fori_loop(0, groups * count, step_body, 0)

    own_plane(0).wait()
    plane_copy(0).wait_recv()
    row_transform_kernel(planes, (0,), ROW_OUTER // 2 + 1)
    gather_blocks(0, 0, near, me, 0, groups)
    send_block(0, 0, near, groups - 1, near - 1, me, 0)
    for place in range(1, 4):
        own_plane(place).wait()
        plane_copy(place).wait_recv()
    row_transform_kernel(planes, (1, 2, 3), ROW_OUTER)
    gather_blocks(1, 0, peers, me, 2, early)

    for swap in range(2):
        far_copy(swap).wait_recv()
    row_transform_kernel(far_plane, (0,), ROW_OUTER // 2 + 1)
    gather_blocks(0, near, near, far_me, 1, groups)
    send_block(0, near, near, groups - 1, near - 1, far_me, 1)

    def send_late(step, carry):
        send_block(1, 0, peers, step // peers, step % peers, me, 2)
        return carry

    lax.fori_loop(early * peers, groups * peers, send_late, 0)

    skip = inner // sub
    thinned = []
    for index, wave in enumerate((row_cos, row_sin)):
        for first in range(0, sub, LANES):
            start = index * inner * (sub // LANES) + first // LANES * inner
            scales[start : start + inner, :] = wave[:, first : first + LANES]
        thinned.append(
            jnp.concatenate(
                [
                    scales[
                        pl.ds(index * inner * (sub // LANES) + first // LANES * inner, sub, skip), :
                    ]
                    for first in range(0, sub, LANES)
                ],
                axis=1,
            )
        )
    store_matrix(*thinned, col_mat_high, col_mat_low)
    spin_copy.wait_recv()
    eye_row = lax.broadcasted_iota(jnp.int32, (LANES, LANES), 0)
    eye_col = lax.broadcasted_iota(jnp.int32, (LANES, LANES), 1)
    eye = (eye_row == eye_col).astype(jnp.float32).astype(jnp.bfloat16)
    column = lax.broadcasted_iota(jnp.int32, (1, degrees), 1)
    bound = jnp.zeros((1, degrees), jnp.int32)
    for j in range(degrees):
        bound = jnp.where(column == j, ells[j], bound)
    for which, ref in ((phi, spins), (other, spin_land)):
        for first in range(0, half, LANES):
            start = pl.multiple_of(which * half + first, LANES)
            span = pl.ds(start, LANES)
            k_id = lax.broadcasted_iota(jnp.int32, (LANES, 1), 0) + start
            keep = jnp.abs(signed(k_id, length)) <= bound
            for spin in range(2):
                value = dot_nt(eye, ref[spin, :, first : first + LANES])
                weights[span, spin * degrees : (spin + 1) * degrees] = jnp.where(keep, value, 0.0)

    low_lanes = lane < BLOCK
    per_plane = half // (LANES * degrees)

    def wide_at(field, pair, j):
        start = (pair % per_plane * degrees + j) * LANES
        if not isinstance(start, int):
            start = pl.multiple_of(start, LANES)
        flat = pair // per_plane
        return 2 * field + flat // 2, flat % 2, slice(None), pl.ds(start, LANES)

    def widen(pair, carry):
        first = weights[pl.ds(2 * pair, sub, peers), :]
        second = weights[pl.ds(2 * pair + 1, sub, peers), :]
        for field in range(2):
            for j in range(degrees):
                at = slice(field * degrees + j, field * degrees + j + 1)
                planes[wide_at(field, pair, j)] = jnp.where(
                    low_lanes, first[:, at], second[:, at]
                ).astype(jnp.bfloat16)
        return carry

    lax.fori_loop(0, peers // split, widen, 0)

    raw_rows = raw.shape[1]
    raw_q = raw_rows // peers
    raw_steps = half // raw_rows
    small = raw_q // 2
    width = small * peers * degrees
    target = lax.broadcasted_iota(jnp.int32, (width, width), 0)
    source_row = lax.broadcasted_iota(jnp.int32, (width, width), 1)
    polar, degree_id = source_row // degrees, source_row % degrees
    wanted = (polar % peers * degrees + degree_id) * small + polar // peers
    order[...] = (wanted == target).astype(jnp.float32).astype(jnp.bfloat16)

    def raw_copy(ref, lanes, step):
        return pltpu.make_async_copy(
            ref.at[pl.ds(pl.multiple_of(step * raw_rows, raw_rows), raw_rows), :, lanes],
            raw.at[step % 2],
            raw_sem.at[step % 2],
        )

    def reorder(ref, lanes, which):
        raw_copy(ref, lanes, 0).start()

        def body(step, carry):
            @pl.when(step + 1 < raw_steps)
            def _():
                raw_copy(ref, lanes, step + 1).start()

            raw_copy(ref, lanes, step).wait()
            base = pl.multiple_of(which * (sub // 2) + step * raw_q, raw_q)
            for wide in range(slots // LANES):
                pieces = []
                for top in range(0, raw_rows, raw_rows // 2):
                    source = raw[
                        step % 2, top : top + raw_rows // 2, :, wide * LANES : (wide + 1) * LANES
                    ].reshape(raw_rows // 2 * degrees, LANES)
                    pieces.append(
                        jnp.dot(order[...], source, preferred_element_type=jnp.float32)
                    )

                def rows_of(k, j):
                    start = (k * degrees + j) * small
                    return jnp.concatenate(
                        [piece[start : start + small] for piece in pieces], axis=0
                    )

                for pair in range(peers // split):
                    for j in range(degrees):
                        first, second = rows_of(2 * pair, j), rows_of(2 * pair + 1, j)
                        span = pl.ds(base, raw_q)
                        table[2 * wide, pair, j, span, :] = jnp.where(
                            low_lanes, first, pltpu.roll(second, BLOCK, 1)
                        ).astype(jnp.bfloat16)
                        table[2 * wide + 1, pair, j, span, :] = jnp.where(
                            low_lanes, pltpu.roll(first, BLOCK, 1), second
                        ).astype(jnp.bfloat16)
            return carry

        lax.fori_loop(0, raw_steps, body, 0)

    reorder(deltas, pl.ds(pl.multiple_of(phi * slots, slots), slots), phi)
    land_copy.wait_recv()
    reorder(land, pl.ds(0, slots), other)

    scale_rows[...] = jnp.zeros_like(scale_rows)

    def column_block(position, carry):
        scalar_turn = (position >= early) & (position < early + groups)
        field = jnp.where(scalar_turn, 0, 1)
        group = jnp.where(
            position < early, position, position - jnp.where(scalar_turn, early, groups)
        )

        @pl.when(field == 0)
        def _():
            def wait_one(n, inner_carry):
                mask = mask_of(near, n)
                peer = flip_bits(me, mask, peers)
                code_copy(0, n, group, mask, peer).wait_recv()
                scale_copy(0, n, group, mask, peer).wait_recv()
                across = flip_bits(peer, near, peers)
                code_copy(0, near + n, group, mask, across).wait_recv()
                scale_copy(0, near + n, group, mask, across).wait_recv()
                return inner_carry

            lax.fori_loop(0, near - 1, wait_one, 0)
            own_copy(0, near - 1, group, me, 0).wait()
            own_copy(0, 2 * near - 1, group, far_me, 1).wait()
            scale_recv[0, group, me] = scale_stage[0, near - 1, group]
            scale_recv[0, group, far_me] = scale_stage[0, 2 * near - 1, group]

        @pl.when(field == 1)
        def _():
            def wait_one(n, inner_carry):
                mask = mask_of(peers, n)
                peer = flip_bits(me, mask, peers)
                code_copy(1, n, group, mask, peer).wait_recv()
                scale_copy(1, n, group, mask, peer).wait_recv()
                return inner_carry

            lax.fori_loop(0, peers - 1, wait_one, 0)
            own_copy(1, peers - 1, group, me, 2).wait()
            scale_recv[1, group, me] = scale_stage[1, peers - 1, group]

        for a in range(peers):
            scale_rows[a : a + 1, :] = scale_recv[field, group, a]
        plain = scale_rows[...]
        own_freq = owner_rows[pl.ds((me * groups + group) // split, 1), :]
        mirrored = ((own_freq & (ROW_OUTER - 1)) > ROW_OUTER // 2) & (field == 0)
        scale_cols[0] = plain.T
        scale_cols[1] = jnp.where(mirrored, -plain, plain).T
        step_rows = 16

        def chunk(step, inner_carry):
            span = pl.ds(pl.multiple_of(step * step_rows, step_rows), step_rows)
            shift_by = group % split * BLOCK + step * step_rows
            scale_span = pl.ds(pl.multiple_of(shift_by, step_rows), step_rows)
            sre, sim = scale_cols[0, scale_span, :], scale_cols[1, scale_span, :]
            for first in range(0, sub, LANES):
                items = []
                for a in range(peers):
                    code = recv[field, a, group, span, first : first + LANES]
                    real = (code >> 16).astype(jnp.float32) * sre[:, a : a + 1]
                    imag = ((code << 16) >> 16).astype(jnp.float32) * sim[:, a : a + 1]
                    items.append((real, imag))
                for k, item in enumerate(butterfly(items)):
                    real, imag = turned(
                        item,
                        col_tc[k : k + 1, first : first + LANES],
                        col_ts[k : k + 1, first : first + LANES],
                    )
                    start = pl.multiple_of(k % fold * BLOCK + step * step_rows, step_rows)
                    place = pl.ds(start, step_rows)
                    split_store(
                        x_high, x_low, (k // fold, place, slice(first, first + LANES)), real
                    )
                    split_store(
                        x_high, x_low,
                        (k // fold, place, slice(sub + first, sub + first + LANES)), imag,
                    )
            return inner_carry

        lax.fori_loop(0, BLOCK // step_rows, chunk, 0)
        total[...] = jnp.zeros_like(total)

        for k4 in range(peers // fold):
            where = (k4, slice(0, rows), slice(0, 2 * sub))
            both = three_dots(col_mat_high, col_mat_low, x_high[where], x_low[where])
            for r in range(fold // split):
                pair = k4 * (fold // split) + r
                span = slice(r * LANES, (r + 1) * LANES)
                real, imag = both[:sub, span], both[sub:, span]
                for j in range(degrees):
                    wide = planes[wide_at(field, pair, j)].astype(jnp.float32)
                    weighted = table[group, pair, j].astype(jnp.float32) * wide
                    for part, value in enumerate((real, imag)):
                        total[2 * j + part] += jnp.sum(
                            (weighted * value).reshape(sub // 8, 8, LANES), axis=0
                        )
        partial = jnp.sum(total[...], axis=1)
        sums[field, group] = partial + pltpu.roll(partial, BLOCK, 1)
        return carry

    lax.fori_loop(0, 2 * groups, column_block, 0)

    for wide in range(slots // LANES):
        slot_freq = signed(owner_rows[pl.ds(me * (slots // LANES) + wide, 1), :], length)
        turns = -slot_freq & 3
        phase_real = jnp.where(turns == 0, 1.0, jnp.where(turns == 2, -1.0, 0.0))
        phase_imag = jnp.where(turns == 1, 1.0, jnp.where(turns == 3, -1.0, 0.0))
        scalar = jnp.where(low_lanes, sums[0, 2 * wide], sums[0, 2 * wide + 1])
        spin = jnp.where(low_lanes, sums[1, 2 * wide], sums[1, 2 * wide + 1])
        for j in range(degrees):
            ell = jnp.full((1, LANES), ells[j], jnp.int32)
            ell_float = ell.astype(jnp.float32)
            weight = jnp.sqrt((2.0 * ell_float + 1.0) / (4.0 * math.pi))
            weight = weight * (2.0 * math.pi / length / length)
            keep = jnp.where(jnp.abs(slot_freq) <= ell, weight, 0.0)
            coupling = priors[j] * jnp.sqrt(ell_float * (ell_float + 1.0)) * (2.0 / length)
            re, im = 2 * j, 2 * j + 1
            inner_real = (-spin[im : im + 1] - coupling * scalar[re : re + 1]) * keep
            inner_imag = (spin[re : re + 1] - coupling * scalar[im : im + 1]) * keep
            span = slice(wide * LANES, (wide + 1) * LANES)
            out_ref[j, 0:1, span] = phase_real * inner_real - phase_imag * inner_imag
            out_ref[j, 1:2, span] = phase_real * inner_imag + phase_imag * inner_real

    for place in range(4):
        plane_copy(place).wait_send()
    for swap in range(2):
        far_copy(swap).wait_send()
    land_copy.wait_send()
    spin_copy.wait_send()

    def finish(count):
        def body(n, carry):
            for group in range(groups):
                for field, base in ((0, 0), (0, near)) if count == near else ((1, 0),):
                    mask = mask_of(count, n)
                    code_copy(field, base + n, group, mask, me).wait_send()
                    scale_copy(field, base + n, group, mask, me).wait_send()
            return carry

        lax.fori_loop(0, count - 1, body, 0)

    finish(near)
    finish(peers)


def wave_tables(row_ids, col_ids, modulus):
    angles = 2.0 * math.pi / modulus * ((row_ids[:, None] * col_ids[None, :]) % modulus)
    return np.cos(angles).astype(np.float32), np.sin(angles).astype(np.float32)


def signed(ids, length):
    return jnp.where(ids < length // 2, ids, ids - length)


def pipeline_call(peers, maps, deltas, spins, owner_map, ell_index, prior):
    fields_in, rows_all, half = maps.shape
    rows = rows_all // 2
    length = 2 * half
    slots = deltas.shape[2] // 2
    degrees = deltas.shape[1]
    groups = slots // BLOCK
    inner = length // ROW_OUTER
    sub = length // peers
    ids = np.arange(length)
    row_cos, row_sin = wave_tables(ids[:inner], ids[:inner], inner)
    row_tc, row_ts = wave_tables(ids[:ROW_OUTER], ids[:inner], length)
    col_tc, col_ts = wave_tables(ids[:peers], ids[:sub], length)
    small = 8
    raw_rows = 2 * small * peers
    width = small * peers * degrees
    bf, f32 = jnp.bfloat16, jnp.float32
    vmem = pl.BlockSpec(memory_space=pltpu.VMEM)
    smem = pl.BlockSpec(memory_space=pltpu.SMEM)
    anywhere = pl.BlockSpec(memory_space=pl.ANY)
    dma = pltpu.SemaphoreType.DMA
    return pl.pallas_call(
        functools.partial(pipeline_kernel, peers),
        in_specs=[anywhere, anywhere, vmem, smem, vmem, smem, smem] + [vmem] * 6,
        out_specs=[vmem, anywhere],
        out_shape=[
            jax.ShapeDtypeStruct((degrees, 2, slots), f32),
            jax.ShapeDtypeStruct((half, degrees, slots), bf),
        ],
        scratch_shapes=[
            pltpu.VMEM((fields_in, 2, rows, half), bf),
            pltpu.VMEM((1, 2, rows, half), bf),
            pltpu.VMEM((ROW_OUTER, rows, 2 * inner), bf),
            pltpu.VMEM((ROW_OUTER, rows, 2 * inner), bf),
            pltpu.VMEM((2 * inner, 2 * inner), bf),
            pltpu.VMEM((2 * inner, 2 * inner), bf),
            pltpu.VMEM((2 * sub, 2 * sub), bf),
            pltpu.VMEM((2 * sub, 2 * sub), bf),
            pltpu.VMEM((length, rows), jnp.int32),
            pltpu.VMEM((length, LANES), f32),
            pltpu.VMEM((2, peers, groups, BLOCK, rows), jnp.int32),
            pltpu.VMEM((2, peers, groups, 1, LANES), f32),
            pltpu.VMEM((2, peers, groups, BLOCK, rows), jnp.int32),
            pltpu.VMEM((2, groups, peers, 1, LANES), f32),
            pltpu.VMEM((groups, peers * BLOCK // LANES, degrees, sub, LANES), bf),
            pltpu.VMEM((2, raw_rows, degrees, slots), bf),
            pltpu.VMEM((width, width), bf),
            pltpu.VMEM(spins.shape, bf),
            pltpu.VMEM((length, 2 * degrees), f32),
            pltpu.VMEM((LANES, LANES), f32),
            pltpu.VMEM((2, LANES, LANES), f32),
            pltpu.VMEM((2 * degrees, 8, LANES), f32),
            pltpu.VMEM((2, groups, 2 * degrees, LANES), f32),
            dma((fields_in,)),
            dma((fields_in,)),
            dma((fields_in,)),
            dma((2,)),
            dma((2,)),
            dma,
            dma,
            dma,
            dma,
            dma((2,)),
            dma((2, peers, groups)),
            dma((2, peers, groups)),
            dma((2, peers, groups)),
            dma((2, peers, groups)),
            dma((3, groups)),
        ],
        compiler_params=pltpu.CompilerParams(
            vmem_limit_bytes=VMEM_LIMIT, collective_id=0, has_side_effects=True
        ),
    )(
        maps, deltas, spins, owner_map, owner_map.reshape(-1, LANES), ell_index, prior,
        row_cos, row_sin, row_tc, row_ts, col_tc, col_ts,
    )[0]


def on_device(maps, deltas, spin_rows, ell_index, owner_map, prior):
    peers = lax.axis_size("theta") * lax.axis_size("phi")
    spins = spin_rows.transpose(1, 2, 0)
    return pipeline_call(peers, maps, deltas, spins, owner_map, ell_index, prior)


def solution(mesh):
    owner_count = mesh.shape["theta"] * mesh.shape["phi"]
    paired = mesh.shape["phi"] == 2 and owner_count == 16
    body = on_device if paired else on_device_general
    placed = (
        P("grp", "theta", "phi"),
        P("phi", None, "theta"),
        P("phi", None, None),
        P(),
        P(),
        P(),
    )
    return jax.shard_map(
        body,
        mesh=mesh,
        in_specs=placed,
        out_specs=P("grp", None, ("theta", "phi")),
        check_vma=False,
    )
```

```python
import functools
import math

import jax
import jax.numpy as jnp
import numpy as np
from jax import lax
from jax.experimental import pallas as pl
from jax.experimental.pallas import tpu as pltpu
from jax.sharding import PartitionSpec as P


def exact_einsum(form, table, operand):
    return jnp.einsum(form, table, operand, precision=lax.Precision.HIGHEST)


def angle_tables(row_count, start, count, modulus):
    freq_rows = jnp.arange(row_count, dtype=jnp.int32)
    sample_cols = start + jnp.arange(count, dtype=jnp.int32)
    angles = (
        2.0
        * math.pi
        / modulus
        * jnp.mod(freq_rows[:, None] * sample_cols[None, :], modulus).astype(jnp.float32)
    )
    return (jnp.cos(angles), jnp.sin(angles))


def row_transform(real_part, imag_part, outer_len, inner_len):
    row_count = real_part.shape[0]
    length = outer_len * inner_len
    cos_a, sin_a = angle_tables(outer_len, 0, outer_len, outer_len)
    real_blocks = real_part.reshape(row_count, outer_len, inner_len)
    section_real = exact_einsum("ka,rab->rkb", cos_a, real_blocks)
    section_imag = -exact_einsum("ka,rab->rkb", sin_a, real_blocks)
    if imag_part is not None:
        imag_blocks = imag_part.reshape(row_count, outer_len, inner_len)
        section_real = section_real + exact_einsum("ka,rab->rkb", sin_a, imag_blocks)
        section_imag = section_imag + exact_einsum("ka,rab->rkb", cos_a, imag_blocks)
    cos_t, sin_t = angle_tables(outer_len, 0, inner_len, length)
    turned_real = section_real * cos_t + section_imag * sin_t
    turned_imag = section_imag * cos_t - section_real * sin_t
    cos_b, sin_b = angle_tables(inner_len, 0, inner_len, inner_len)
    out_real = exact_einsum("qb,rkb->rqk", cos_b, turned_real) + exact_einsum(
        "qb,rkb->rqk", sin_b, turned_imag
    )
    out_imag = exact_einsum("qb,rkb->rqk", cos_b, turned_imag) - exact_einsum(
        "qb,rkb->rqk", sin_b, turned_real
    )
    return (out_real.reshape(row_count, length), out_imag.reshape(row_count, length))


def column_transform(real_part, imag_part, outer_len, inner_len, start):
    fields = real_part.shape[0]
    count = real_part.shape[2]
    slots = real_part.shape[3]
    length = outer_len * inner_len
    cos_a, sin_a = angle_tables(outer_len, 0, outer_len, outer_len)
    section_real = exact_einsum("ka,fabm->fkbm", cos_a, real_part) + exact_einsum(
        "ka,fabm->fkbm", sin_a, imag_part
    )
    section_imag = exact_einsum("ka,fabm->fkbm", cos_a, imag_part) - exact_einsum(
        "ka,fabm->fkbm", sin_a, real_part
    )
    cos_t, sin_t = angle_tables(outer_len, start, count, length)
    cos_t = cos_t[:, :, None]
    sin_t = sin_t[:, :, None]
    turned_real = section_real * cos_t + section_imag * sin_t
    turned_imag = section_imag * cos_t - section_real * sin_t
    cos_b, sin_b = angle_tables(inner_len, start, count, inner_len)
    out_real = exact_einsum("qb,fkbm->fqkm", cos_b, turned_real) + exact_einsum(
        "qb,fkbm->fqkm", sin_b, turned_imag
    )
    out_imag = exact_einsum("qb,fkbm->fqkm", cos_b, turned_imag) - exact_einsum(
        "qb,fkbm->fqkm", sin_b, turned_real
    )
    return (out_real.reshape(fields, length, slots), out_imag.reshape(fields, length, slots))


def accumulate(spectrum_block, table_block, spin_block, length, ell_index):
    count = table_block.shape[0]
    positions = jnp.arange(count, dtype=jnp.int32)
    freq = jnp.where(positions < length // 2, positions, positions - length)
    terms = []
    for degree in range(table_block.shape[1]):
        keep_rows = (jnp.abs(freq) <= ell_index[degree]).astype(jnp.float32)
        row_weights = spin_block[:, :, degree].astype(jnp.float32).T * keep_rows[None, :]
        table = table_block[:, degree, :].astype(jnp.float32)
        terms.append(
            jnp.einsum(
                "fk,ks,xfks->fxs",
                row_weights,
                table,
                spectrum_block,
                precision=lax.Precision.HIGHEST,
            )
        )
    return jnp.stack(terms)


def on_device_general(maps, deltas, spin_rows, ell_index, owner_map, prior):
    theta_count = lax.axis_size("theta")
    phi_count = lax.axis_size("phi")
    length = maps.shape[2] * phi_count
    values = maps.astype(jnp.float32)
    planes = jnp.stack([values[0], values[1] * values[2], values[1] * values[3]])
    row_planes = lax.all_to_all(planes, "phi", split_axis=1, concat_axis=2, tiled=True)
    inner_len = length // theta_count
    spectra = [
        row_transform(row_planes[0], None, theta_count, inner_len),
        row_transform(row_planes[1], row_planes[2], theta_count, inner_len),
    ]
    stacked = jnp.stack(
        [
            jnp.stack([spectrum[0] for spectrum in spectra]),
            jnp.stack([spectrum[1] for spectrum in spectra]),
        ]
    )
    permuted = jnp.take(stacked, owner_map, axis=3)
    columns = lax.all_to_all(permuted, "theta", split_axis=3, concat_axis=2, tiled=True)
    fields = columns.shape[1]
    slots = columns.shape[3]
    sub_rows = columns.shape[2] // theta_count
    blocks = columns.reshape(2, fields, theta_count, sub_rows, slots)
    row_start = lax.axis_index("phi") * sub_rows
    spec_real, spec_imag = column_transform(blocks[0], blocks[1], theta_count, inner_len, row_start)
    combined = jnp.stack([spec_real, spec_imag])
    totals = accumulate(
        combined,
        lax.all_gather(deltas, "phi", axis=0, tiled=True),
        lax.all_gather(spin_rows, "phi", axis=0, tiled=True),
        length,
        ell_index,
    )
    shares = lax.psum_scatter(totals, "phi", scatter_dimension=3, tiled=True)
    share_count = shares.shape[3]
    slot_start = lax.axis_index("theta") * slots + lax.axis_index("phi") * share_count
    share_ids = lax.dynamic_slice_in_dim(owner_map, slot_start, share_count)
    slot_freq = jnp.where(share_ids < length // 2, share_ids, share_ids - length)
    ell_float = ell_index.astype(jnp.float32)
    weight = 2.0 * math.pi / length * jnp.sqrt((2.0 * ell_float + 1.0) / (4.0 * math.pi)) / length
    keep_slots = (jnp.abs(slot_freq)[None, :] <= ell_index[:, None]).astype(jnp.float32) * weight[
        :, None
    ]
    scalar_real = shares[:, 0, 0] * keep_slots
    scalar_imag = shares[:, 0, 1] * keep_slots
    spin_real = shares[:, 1, 0] * keep_slots
    spin_imag = shares[:, 1, 1] * keep_slots
    coupling = (prior * jnp.sqrt(ell_float * (ell_float + 1.0)) / (length // 2))[:, None]
    inner_real = -spin_imag - coupling * scalar_real
    inner_imag = spin_real - coupling * scalar_imag
    turns = jnp.mod(-slot_freq, 4)
    phase_real = jnp.where(turns == 0, 1.0, jnp.where(turns == 2, -1.0, 0.0)).astype(jnp.float32)[
        None, :
    ]
    phase_imag = jnp.where(turns == 1, 1.0, jnp.where(turns == 3, -1.0, 0.0)).astype(jnp.float32)[
        None, :
    ]
    out_real = phase_real * inner_real - phase_imag * inner_imag
    out_imag = phase_real * inner_imag + phase_imag * inner_real
    return jnp.stack([out_real, out_imag], axis=1)


ROW_OUTER = 8
LANES = 128
BLOCK = 64
VMEM_LIMIT = 67043328
CODE_TOP = 32767.0
MESH = pl.DeviceIdType.MESH


def cplx_add(x, y):
    return tuple(b if a is None else a if b is None else a + b for a, b in zip(x, y))


def cplx_sub(x, y):
    return tuple(
        (None if b is None else -b) if a is None else a if b is None else a - b
        for a, b in zip(x, y)
    )


def turn(x, step, count):
    real, imag = x
    if step == 0:
        return x
    if 4 * step == count:
        return (imag, None if real is None else -real)
    cos_v = math.cos(2.0 * math.pi * step / count)
    sin_v = math.sin(2.0 * math.pi * step / count)
    if imag is None:
        return (real * cos_v, real * -sin_v)
    if 8 * step == count:
        return ((real + imag) * cos_v, (imag - real) * cos_v)
    if 8 * step == 3 * count:
        return ((imag - real) * sin_v, (real + imag) * -sin_v)
    return (real * cos_v + imag * sin_v, imag * cos_v - real * sin_v)


def butterfly(items):
    count = len(items)
    if count == 1:
        return items
    even, odd = butterfly(items[::2]), butterfly(items[1::2])
    turned = [turn(x, step, count) for step, x in enumerate(odd)]
    return [cplx_add(a, b) for a, b in zip(even, turned)] + [
        cplx_sub(a, b) for a, b in zip(even, turned)
    ]


def split_store(high, low, where, value):
    top = value.astype(jnp.bfloat16)
    high[where] = top
    low[where] = (value - top.astype(jnp.float32)).astype(jnp.bfloat16)


def store_matrix(cos_v, sin_v, high, low):
    size = cos_v.shape[0]
    first, second = slice(0, size), slice(size, 2 * size)
    split_store(high, low, (first, first), cos_v)
    split_store(high, low, (first, second), sin_v)
    split_store(high, low, (second, first), -sin_v)
    split_store(high, low, (second, second), cos_v)


def dot_nt(left, right):
    return lax.dot_general(
        left, right, (((1,), (1,)), ((), ())), preferred_element_type=jnp.float32
    )


def three_dots(mat_high, mat_low, high, low):
    return dot_nt(mat_high[...], high) + dot_nt(mat_high[...], low) + dot_nt(mat_low[...], high)


def turned(item, cos_v, sin_v):
    real, imag = item
    if imag is None:
        return real * cos_v, real * -sin_v
    return real * cos_v + imag * sin_v, imag * cos_v - real * sin_v


def flip_bits(value, mask, count):
    result, bit = 0, 1
    while bit < count:
        result = result + ((value // bit + mask // bit) % 2) * bit
        bit *= 2
    return result


def pipeline_kernel(
    peers, maps, deltas, spins, owner, owner_rows, ells, priors, row_cos, row_sin, row_tc, row_ts,
    col_tc, col_ts, out_ref, land,
    planes, far_plane, x_high, x_low, row_mat_high, row_mat_low, col_mat_high, col_mat_low,
    codes, scales, stage, scale_stage, recv, scale_recv, table, raw, order, spin_land, weights,
    scale_rows, scale_cols, total, sums, plane_send, plane_recv, plane_own, far_send, far_recv,
    land_send, land_recv, spin_send, spin_recv, raw_sem, code_send, code_recv, scale_send,
    scale_sem, own_sem,
):
    theta, phi = lax.axis_index("theta"), lax.axis_index("phi")
    me = theta * 2 + phi
    other = 1 - phi
    rows = planes.shape[2]
    half = planes.shape[3]
    length = 2 * half
    inner = row_cos.shape[0]
    sub = col_tc.shape[1]
    groups = recv.shape[2]
    degrees = deltas.shape[1]
    slots = groups * BLOCK
    fold = rows // BLOCK
    early = 1
    split = LANES // BLOCK
    near = peers // 2
    far_me = flip_bits(me, near, peers)
    parts_per_half = half // inner

    def device(index):
        return {"theta": index // 2, "phi": index % 2}

    barrier = pltpu.get_barrier_semaphore()
    for mask in range(1, peers):
        pl.semaphore_signal(
            barrier, inc=1, device_id=device(flip_bits(me, mask, peers)), device_id_type=MESH
        )
    pl.semaphore_wait(barrier, peers - 1)

    def far_copy(swap):
        target = (phi + swap) % 2
        return pltpu.make_async_remote_copy(
            src_ref=maps.at[0, pl.ds(pl.multiple_of(target * rows, rows), rows), :],
            dst_ref=far_plane.at[0, swap],
            send_sem=far_send.at[swap],
            recv_sem=far_recv.at[swap],
            device_id=device(flip_bits(me, near + swap, peers)),
            device_id_type=MESH,
        )

    def plane_copy(place):
        return pltpu.make_async_remote_copy(
            src_ref=maps.at[place, pl.ds(pl.multiple_of(other * rows, rows), rows), :],
            dst_ref=planes.at[place, 1],
            send_sem=plane_send.at[place],
            recv_sem=plane_recv.at[place],
            device_id={"phi": other},
            device_id_type=MESH,
        )

    def own_plane(place):
        return pltpu.make_async_copy(
            maps.at[place, pl.ds(pl.multiple_of(phi * rows, rows), rows), :],
            planes.at[place, 0],
            plane_own.at[place],
        )

    for swap in range(2):
        far_copy(swap).start()
    for place in range(4):
        plane_copy(place).start()
        own_plane(place).start()
    land_copy = pltpu.make_async_remote_copy(
        src_ref=deltas.at[:, :, pl.ds(pl.multiple_of(other * slots, slots), slots)],
        dst_ref=land,
        send_sem=land_send,
        recv_sem=land_recv,
        device_id={"phi": other},
        device_id_type=MESH,
    )
    land_copy.start()
    spin_copy = pltpu.make_async_remote_copy(
        src_ref=spins,
        dst_ref=spin_land,
        send_sem=spin_send,
        recv_sem=spin_recv,
        device_id={"phi": other},
        device_id_type=MESH,
    )
    spin_copy.start()
    store_matrix(row_cos[...], row_sin[...], row_mat_high, row_mat_low)

    sign = (1 - 2 * phi).astype(jnp.float32)

    def row_transform_kernel(source, places_in, kept):
        step_rows = 16

        def chunk(step, carry):
            span = pl.ds(pl.multiple_of(step * step_rows, step_rows), step_rows)
            for first in range(0, inner, LANES):

                def part(place, a):
                    start = (a % parts_per_half) * inner + first
                    return source[
                        place, a // parts_per_half, span, start : start + LANES
                    ].astype(jnp.float32)

                items = []
                for a in range(ROW_OUTER):
                    if len(places_in) == 1:
                        items.append((part(places_in[0], a), None))
                    else:
                        base = part(places_in[0], a)
                        items.append((base * part(places_in[1], a), base * part(places_in[2], a)))
                done = butterfly(items)
                for k in range(kept):
                    cos_k = row_tc[k : k + 1, first : first + LANES]
                    sin_k = row_ts[k : k + 1, first : first + LANES]
                    if k % 2:
                        cos_k, sin_k = cos_k * sign, sin_k * sign
                    real, imag = turned(done[k], cos_k, sin_k)
                    split_store(x_high, x_low, (k, span, slice(first, first + LANES)), real)
                    split_store(
                        x_high, x_low, (k, span, slice(inner + first, inner + first + LANES)), imag
                    )
            return carry

        lax.fori_loop(0, rows // step_rows, chunk, 0)

        def block(k, carry):
            both = three_dots(row_mat_high, row_mat_low, x_high[k], x_low[k])
            real, imag = both[:inner], both[inner:]
            top = jnp.max(jnp.maximum(jnp.abs(real), jnp.abs(imag)), axis=1, keepdims=True)
            top = jnp.maximum(top, 1e-30)
            factor = CODE_TOP / top
            code_real = jnp.round(real * factor).astype(jnp.int32)
            code_imag = jnp.round(imag * factor).astype(jnp.int32)
            span = pl.ds(pl.multiple_of(k * inner, inner), inner)
            codes[span, :] = (code_real << 16) | (code_imag & 0xFFFF)
            scales[span, :] = jnp.broadcast_to(top * (1.0 / CODE_TOP), (inner, LANES))
            return carry

        lax.fori_loop(0, kept, block, 0)

    def mask_of(count, n):
        if count == peers:
            return peers - 1 - n // 2 - near * (n % 2)
        return count - 1 - n

    def code_copy(field, slot, group, mask, source):
        return pltpu.make_async_remote_copy(
            src_ref=stage.at[field, slot, group],
            dst_ref=recv.at[field, source, group],
            send_sem=code_send.at[field, slot, group],
            recv_sem=code_recv.at[field, source, group],
            device_id=device(flip_bits(me, mask, peers)),
            device_id_type=MESH,
        )

    def scale_copy(field, slot, group, mask, source):
        return pltpu.make_async_remote_copy(
            src_ref=scale_stage.at[field, slot, group],
            dst_ref=scale_recv.at[field, group, source],
            send_sem=scale_send.at[field, slot, group],
            recv_sem=scale_sem.at[field, source, group],
            device_id=device(flip_bits(me, mask, peers)),
            device_id_type=MESH,
        )

    def own_copy(field, slot, group, source, which):
        return pltpu.make_async_copy(
            stage.at[field, slot, group], recv.at[field, source, group], own_sem.at[which, group]
        )

    lane = lax.broadcasted_iota(jnp.int32, (1, LANES), 1)
    unroll = 16
    shift = ROW_OUTER.bit_length() - 1

    def send_block(field, base, count, group, n, source, which):
        @pl.when(n != count - 1)
        def _():
            mask = mask_of(count, n)
            code_copy(field, base + n, group, mask, source).start()
            scale_copy(field, base + n, group, mask, source).start()

        @pl.when(n == count - 1)
        def _():
            own_copy(field, base + n, group, source, which).start()

    def gather_blocks(field, base, count, source, which, sent_groups):
        def step_body(step, carry):
            group, n = step // count, step % count
            dest = flip_bits(me, mask_of(count, n), peers)
            first = dest * slots + group * BLOCK
            shown = lane - group % split * BLOCK

            def rows_body(g, acc):
                start = pl.multiple_of(g * unroll, unroll)
                for u in range(unroll):
                    freq = owner[first + start + u]
                    if field == 0:
                        mirrored = (freq & (ROW_OUTER - 1)) > ROW_OUTER // 2
                        freq = jnp.where(mirrored, length - freq, freq)
                    where = (freq & (ROW_OUTER - 1)) * inner + (freq >> shift)
                    stage[field, base + n, group, pl.ds(start + u, 1), :] = codes[
                        pl.ds(where, 1), :
                    ]
                    acc = jnp.where(shown == start + u, scales[pl.ds(where, 1), :], acc)
                return acc

            acc = lax.fori_loop(0, BLOCK // unroll, rows_body, jnp.zeros((1, LANES), jnp.float32))
            scale_stage[field, base + n, group] = acc

            @pl.when((step > 0) & (step <= sent_groups * count))
            def _():
                before = step - 1
                send_block(field, base, count, before // count, before % count, source, which)

            return carry

        lax.fori_loop(0, groups * count, step_body, 0)

    own_plane(0).wait()
    plane_copy(0).wait_recv()
    row_transform_kernel(planes, (0,), ROW_OUTER // 2 + 1)
    gather_blocks(0, 0, near, me, 0, groups)
    send_block(0, 0, near, groups - 1, near - 1, me, 0)
    for place in range(1, 4):
        own_plane(place).wait()
        plane_copy(place).wait_recv()
    row_transform_kernel(planes, (1, 2, 3), ROW_OUTER)
    gather_blocks(1, 0, peers, me, 2, early)

    for swap in range(2):
        far_copy(swap).wait_recv()
    row_transform_kernel(far_plane, (0,), ROW_OUTER // 2 + 1)
    gather_blocks(0, near, near, far_me, 1, groups)
    send_block(0, near, near, groups - 1, near - 1, far_me, 1)

    def send_late(step, carry):
        send_block(1, 0, peers, step // peers, step % peers, me, 2)
        return carry

    lax.fori_loop(early * peers, groups * peers, send_late, 0)

    skip = inner // sub
    thinned = []
    for index, wave in enumerate((row_cos, row_sin)):
        for first in range(0, sub, LANES):
            start = index * inner * (sub // LANES) + first // LANES * inner
            scales[start : start + inner, :] = wave[:, first : first + LANES]
        thinned.append(
            jnp.concatenate(
                [
                    scales[
                        pl.ds(index * inner * (sub // LANES) + first // LANES * inner, sub, skip), :
                    ]
                    for first in range(0, sub, LANES)
                ],
                axis=1,
            )
        )
    store_matrix(*thinned, col_mat_high, col_mat_low)
    spin_copy.wait_recv()
    eye_row = lax.broadcasted_iota(jnp.int32, (LANES, LANES), 0)
    eye_col = lax.broadcasted_iota(jnp.int32, (LANES, LANES), 1)
    eye = (eye_row == eye_col).astype(jnp.float32).astype(jnp.bfloat16)
    column = lax.broadcasted_iota(jnp.int32, (1, degrees), 1)
    bound = jnp.zeros((1, degrees), jnp.int32)
    for j in range(degrees):
        bound = jnp.where(column == j, ells[j], bound)
    for which, ref in ((phi, spins), (other, spin_land)):
        for first in range(0, half, LANES):
            start = pl.multiple_of(which * half + first, LANES)
            span = pl.ds(start, LANES)
            k_id = lax.broadcasted_iota(jnp.int32, (LANES, 1), 0) + start
            keep = jnp.abs(signed(k_id, length)) <= bound
            for spin in range(2):
                value = dot_nt(eye, ref[spin, :, first : first + LANES])
                weights[span, spin * degrees : (spin + 1) * degrees] = jnp.where(keep, value, 0.0)

    low_lanes = lane < BLOCK
    per_plane = half // (LANES * degrees)

    def wide_at(field, pair, j):
        start = (pair % per_plane * degrees + j) * LANES
        if not isinstance(start, int):
            start = pl.multiple_of(start, LANES)
        flat = pair // per_plane
        return 2 * field + flat // 2, flat % 2, slice(None), pl.ds(start, LANES)

    def widen(pair, carry):
        first = weights[pl.ds(2 * pair, sub, peers), :]
        second = weights[pl.ds(2 * pair + 1, sub, peers), :]
        for field in range(2):
            for j in range(degrees):
                at = slice(field * degrees + j, field * degrees + j + 1)
                planes[wide_at(field, pair, j)] = jnp.where(
                    low_lanes, first[:, at], second[:, at]
                ).astype(jnp.bfloat16)
        return carry

    lax.fori_loop(0, peers // split, widen, 0)

    raw_rows = raw.shape[1]
    raw_q = raw_rows // peers
    raw_steps = half // raw_rows
    small = raw_q // 2
    width = small * peers * degrees
    target = lax.broadcasted_iota(jnp.int32, (width, width), 0)
    source_row = lax.broadcasted_iota(jnp.int32, (width, width), 1)
    polar, degree_id = source_row // degrees, source_row % degrees
    wanted = (polar % peers * degrees + degree_id) * small + polar // peers
    order[...] = (wanted == target).astype(jnp.float32).astype(jnp.bfloat16)

    def raw_copy(ref, lanes, step):
        return pltpu.make_async_copy(
            ref.at[pl.ds(pl.multiple_of(step * raw_rows, raw_rows), raw_rows), :, lanes],
            raw.at[step % 2],
            raw_sem.at[step % 2],
        )

    def reorder(ref, lanes, which):
        raw_copy(ref, lanes, 0).start()

        def body(step, carry):
            @pl.when(step + 1 < raw_steps)
            def _():
                raw_copy(ref, lanes, step + 1).start()

            raw_copy(ref, lanes, step).wait()
            base = pl.multiple_of(which * (sub // 2) + step * raw_q, raw_q)
            for wide in range(slots // LANES):
                pieces = []
                for top in range(0, raw_rows, raw_rows // 2):
                    source = raw[
                        step % 2, top : top + raw_rows // 2, :, wide * LANES : (wide + 1) * LANES
                    ].reshape(raw_rows // 2 * degrees, LANES)
                    pieces.append(
                        jnp.dot(order[...], source, preferred_element_type=jnp.float32)
                    )

                def rows_of(k, j):
                    start = (k * degrees + j) * small
                    return jnp.concatenate(
                        [piece[start : start + small] for piece in pieces], axis=0
                    )

                for pair in range(peers // split):
                    for j in range(degrees):
                        first, second = rows_of(2 * pair, j), rows_of(2 * pair + 1, j)
                        span = pl.ds(base, raw_q)
                        table[2 * wide, pair, j, span, :] = jnp.where(
                            low_lanes, first, pltpu.roll(second, BLOCK, 1)
                        ).astype(jnp.bfloat16)
                        table[2 * wide + 1, pair, j, span, :] = jnp.where(
                            low_lanes, pltpu.roll(first, BLOCK, 1), second
                        ).astype(jnp.bfloat16)
            return carry

        lax.fori_loop(0, raw_steps, body, 0)

    reorder(deltas, pl.ds(pl.multiple_of(phi * slots, slots), slots), phi)
    land_copy.wait_recv()
    reorder(land, pl.ds(0, slots), other)

    scale_rows[...] = jnp.zeros_like(scale_rows)

    def column_block(position, carry):
        scalar_turn = (position >= early) & (position < early + groups)
        field = jnp.where(scalar_turn, 0, 1)
        group = jnp.where(
            position < early, position, position - jnp.where(scalar_turn, early, groups)
        )

        @pl.when(field == 0)
        def _():
            def wait_one(n, inner_carry):
                mask = mask_of(near, n)
                peer = flip_bits(me, mask, peers)
                code_copy(0, n, group, mask, peer).wait_recv()
                scale_copy(0, n, group, mask, peer).wait_recv()
                across = flip_bits(peer, near, peers)
                code_copy(0, near + n, group, mask, across).wait_recv()
                scale_copy(0, near + n, group, mask, across).wait_recv()
                return inner_carry

            lax.fori_loop(0, near - 1, wait_one, 0)
            own_copy(0, near - 1, group, me, 0).wait()
            own_copy(0, 2 * near - 1, group, far_me, 1).wait()
            scale_recv[0, group, me] = scale_stage[0, near - 1, group]
            scale_recv[0, group, far_me] = scale_stage[0, 2 * near - 1, group]

        @pl.when(field == 1)
        def _():
            def wait_one(n, inner_carry):
                mask = mask_of(peers, n)
                peer = flip_bits(me, mask, peers)
                code_copy(1, n, group, mask, peer).wait_recv()
                scale_copy(1, n, group, mask, peer).wait_recv()
                return inner_carry

            lax.fori_loop(0, peers - 1, wait_one, 0)
            own_copy(1, peers - 1, group, me, 2).wait()
            scale_recv[1, group, me] = scale_stage[1, peers - 1, group]

        for a in range(peers):
            scale_rows[a : a + 1, :] = scale_recv[field, group, a]
        plain = scale_rows[...]
        own_freq = owner_rows[pl.ds((me * groups + group) // split, 1), :]
        mirrored = ((own_freq & (ROW_OUTER - 1)) > ROW_OUTER // 2) & (field == 0)
        scale_cols[0] = plain.T
        scale_cols[1] = jnp.where(mirrored, -plain, plain).T
        step_rows = 16

        def chunk(step, inner_carry):
            span = pl.ds(pl.multiple_of(step * step_rows, step_rows), step_rows)
            shift_by = group % split * BLOCK + step * step_rows
            scale_span = pl.ds(pl.multiple_of(shift_by, step_rows), step_rows)
            sre, sim = scale_cols[0, scale_span, :], scale_cols[1, scale_span, :]
            for first in range(0, sub, LANES):
                items = []
                for a in range(peers):
                    code = recv[field, a, group, span, first : first + LANES]
                    real = (code >> 16).astype(jnp.float32) * sre[:, a : a + 1]
                    imag = ((code << 16) >> 16).astype(jnp.float32) * sim[:, a : a + 1]
                    items.append((real, imag))
                for k, item in enumerate(butterfly(items)):
                    real, imag = turned(
                        item,
                        col_tc[k : k + 1, first : first + LANES],
                        col_ts[k : k + 1, first : first + LANES],
                    )
                    start = pl.multiple_of(k % fold * BLOCK + step * step_rows, step_rows)
                    place = pl.ds(start, step_rows)
                    split_store(
                        x_high, x_low, (k // fold, place, slice(first, first + LANES)), real
                    )
                    split_store(
                        x_high, x_low,
                        (k // fold, place, slice(sub + first, sub + first + LANES)), imag,
                    )
            return inner_carry

        lax.fori_loop(0, BLOCK // step_rows, chunk, 0)
        total[...] = jnp.zeros_like(total)

        for k4 in range(peers // fold):
            where = (k4, slice(0, rows), slice(0, 2 * sub))
            both = three_dots(col_mat_high, col_mat_low, x_high[where], x_low[where])
            for r in range(fold // split):
                pair = k4 * (fold // split) + r
                span = slice(r * LANES, (r + 1) * LANES)
                real, imag = both[:sub, span], both[sub:, span]
                for j in range(degrees):
                    wide = planes[wide_at(field, pair, j)].astype(jnp.float32)
                    weighted = table[group, pair, j].astype(jnp.float32) * wide
                    for part, value in enumerate((real, imag)):
                        total[2 * j + part] += jnp.sum(
                            (weighted * value).reshape(sub // 8, 8, LANES), axis=0
                        )
        partial = jnp.sum(total[...], axis=1)
        sums[field, group] = partial + pltpu.roll(partial, BLOCK, 1)
        return carry

    lax.fori_loop(0, 2 * groups, column_block, 0)

    for wide in range(slots // LANES):
        slot_freq = signed(owner_rows[pl.ds(me * (slots // LANES) + wide, 1), :], length)
        turns = -slot_freq & 3
        phase_real = jnp.where(turns == 0, 1.0, jnp.where(turns == 2, -1.0, 0.0))
        phase_imag = jnp.where(turns == 1, 1.0, jnp.where(turns == 3, -1.0, 0.0))
        scalar = jnp.where(low_lanes, sums[0, 2 * wide], sums[0, 2 * wide + 1])
        spin = jnp.where(low_lanes, sums[1, 2 * wide], sums[1, 2 * wide + 1])
        for j in range(degrees):
            ell = jnp.full((1, LANES), ells[j], jnp.int32)
            ell_float = ell.astype(jnp.float32)
            weight = jnp.sqrt((2.0 * ell_float + 1.0) / (4.0 * math.pi))
            weight = weight * (2.0 * math.pi / length / length)
            keep = jnp.where(jnp.abs(slot_freq) <= ell, weight, 0.0)
            coupling = priors[j] * jnp.sqrt(ell_float * (ell_float + 1.0)) * (2.0 / length)
            re, im = 2 * j, 2 * j + 1
            inner_real = (-spin[im : im + 1] - coupling * scalar[re : re + 1]) * keep
            inner_imag = (spin[re : re + 1] - coupling * scalar[im : im + 1]) * keep
            span = slice(wide * LANES, (wide + 1) * LANES)
            out_ref[j, 0:1, span] = phase_real * inner_real - phase_imag * inner_imag
            out_ref[j, 1:2, span] = phase_real * inner_imag + phase_imag * inner_real

    for place in range(4):
        plane_copy(place).wait_send()
    for swap in range(2):
        far_copy(swap).wait_send()
    land_copy.wait_send()
    spin_copy.wait_send()

    def finish(count):
        def body(n, carry):
            for group in range(groups):
                for field, base in ((0, 0), (0, near)) if count == near else ((1, 0),):
                    mask = mask_of(count, n)
                    code_copy(field, base + n, group, mask, me).wait_send()
                    scale_copy(field, base + n, group, mask, me).wait_send()
            return carry

        lax.fori_loop(0, count - 1, body, 0)

    finish(near)
    finish(peers)


def wave_tables(row_ids, col_ids, modulus):
    angles = 2.0 * math.pi / modulus * ((row_ids[:, None] * col_ids[None, :]) % modulus)
    return np.cos(angles).astype(np.float32), np.sin(angles).astype(np.float32)


def signed(ids, length):
    return jnp.where(ids < length // 2, ids, ids - length)


def pipeline_call(peers, maps, deltas, spins, owner_map, ell_index, prior):
    fields_in, rows_all, half = maps.shape
    rows = rows_all // 2
    length = 2 * half
    slots = deltas.shape[2] // 2
    degrees = deltas.shape[1]
    groups = slots // BLOCK
    inner = length // ROW_OUTER
    sub = length // peers
    ids = np.arange(length)
    row_cos, row_sin = wave_tables(ids[:inner], ids[:inner], inner)
    row_tc, row_ts = wave_tables(ids[:ROW_OUTER], ids[:inner], length)
    col_tc, col_ts = wave_tables(ids[:peers], ids[:sub], length)
    small = 8
    raw_rows = 2 * small * peers
    width = small * peers * degrees
    bf, f32 = jnp.bfloat16, jnp.float32
    vmem = pl.BlockSpec(memory_space=pltpu.VMEM)
    smem = pl.BlockSpec(memory_space=pltpu.SMEM)
    anywhere = pl.BlockSpec(memory_space=pl.ANY)
    dma = pltpu.SemaphoreType.DMA
    return pl.pallas_call(
        functools.partial(pipeline_kernel, peers),
        in_specs=[anywhere, anywhere, vmem, smem, vmem, smem, smem] + [vmem] * 6,
        out_specs=[vmem, anywhere],
        out_shape=[
            jax.ShapeDtypeStruct((degrees, 2, slots), f32),
            jax.ShapeDtypeStruct((half, degrees, slots), bf),
        ],
        scratch_shapes=[
            pltpu.VMEM((fields_in, 2, rows, half), bf),
            pltpu.VMEM((1, 2, rows, half), bf),
            pltpu.VMEM((ROW_OUTER, rows, 2 * inner), bf),
            pltpu.VMEM((ROW_OUTER, rows, 2 * inner), bf),
            pltpu.VMEM((2 * inner, 2 * inner), bf),
            pltpu.VMEM((2 * inner, 2 * inner), bf),
            pltpu.VMEM((2 * sub, 2 * sub), bf),
            pltpu.VMEM((2 * sub, 2 * sub), bf),
            pltpu.VMEM((length, rows), jnp.int32),
            pltpu.VMEM((length, LANES), f32),
            pltpu.VMEM((2, peers, groups, BLOCK, rows), jnp.int32),
            pltpu.VMEM((2, peers, groups, 1, LANES), f32),
            pltpu.VMEM((2, peers, groups, BLOCK, rows), jnp.int32),
            pltpu.VMEM((2, groups, peers, 1, LANES), f32),
            pltpu.VMEM((groups, peers * BLOCK // LANES, degrees, sub, LANES), bf),
            pltpu.VMEM((2, raw_rows, degrees, slots), bf),
            pltpu.VMEM((width, width), bf),
            pltpu.VMEM(spins.shape, bf),
            pltpu.VMEM((length, 2 * degrees), f32),
            pltpu.VMEM((LANES, LANES), f32),
            pltpu.VMEM((2, LANES, LANES), f32),
            pltpu.VMEM((2 * degrees, 8, LANES), f32),
            pltpu.VMEM((2, groups, 2 * degrees, LANES), f32),
            dma((fields_in,)),
            dma((fields_in,)),
            dma((fields_in,)),
            dma((2,)),
            dma((2,)),
            dma,
            dma,
            dma,
            dma,
            dma((2,)),
            dma((2, peers, groups)),
            dma((2, peers, groups)),
            dma((2, peers, groups)),
            dma((2, peers, groups)),
            dma((3, groups)),
        ],
        compiler_params=pltpu.CompilerParams(
            vmem_limit_bytes=VMEM_LIMIT, collective_id=0, has_side_effects=True
        ),
    )(
        maps, deltas, spins, owner_map, owner_map.reshape(-1, LANES), ell_index, prior,
        row_cos, row_sin, row_tc, row_ts, col_tc, col_ts,
    )[0]


def on_device(maps, deltas, spin_rows, ell_index, owner_map, prior):
    peers = lax.axis_size("theta") * lax.axis_size("phi")
    spins = spin_rows.transpose(1, 2, 0)
    return pipeline_call(peers, maps, deltas, spins, owner_map, ell_index, prior)


def solution(mesh):
    owner_count = mesh.shape["theta"] * mesh.shape["phi"]
    paired = mesh.shape["phi"] == 2 and owner_count == 16
    body = on_device if paired else on_device_general
    placed = (
        P("grp", "theta", "phi"),
        P("phi", None, "theta"),
        P("phi", None, None),
        P(),
        P(),
        P(),
    )
    return jax.shard_map(
        body,
        mesh=mesh,
        in_specs=placed,
        out_specs=P("grp", None, ("theta", "phi")),
        check_vma=False,
    )
```
